32 devices in a mesh: theta: 8 (over z, core), gz: 4 (over y, x).
Axes of the slice: x: 2, y: 2, z: 4, core: 2. Of those that a mesh axis runs over, the one named last changes fastest.
Arguments:
- velocity: float32 [3, 512, 256, 128], P(None, 'theta', 'gz'), may hold values from -3 to 3
Outputs:
- viscosity_ratio: float32 [512, 256, 128], P('theta', 'gz')
- pressure_modes: float32 [2, 512, 256, 128], P(None, 'gz', 'theta')
The draws below stay inside these ranges and needn't reach their ends.
All inputs are finite; a program needn't handle non-finite values.
Results may differ from the reference program's by a relative error of at most 0.0003.
Values sent between devices are 32-bit elements; how exact they have to be, the bound alone decides.
No kernel may reach another device: no remote copies, remote signals or barrier semaphores. Data moves between devices by JAX's collectives and lax.ppermute only.
A program may use at most 256 MiB of HBM per device.

```python
import math
import jax
import jax.numpy as jnp
from jax import lax

NTH = 512
NZ = 256
NR = 128


def draw_velocity(key, part):
    keys = jax.random.split(jax.random.fold_in(key, 11), 3)
    shape = (3, NTH, NZ, NR)
    theta_pos = (jnp.arange(NTH, dtype=jnp.float32) / NTH)[:, None, None]
    axial_pos = (jnp.arange(NZ, dtype=jnp.float32) / NZ)[None, :, None]
    radius = ((jnp.arange(NR, dtype=jnp.float32) + 0.5) / NR)[None, None, :]
    noise = jnp.clip(jax.random.normal(keys[0], shape, jnp.float32), -5.0, 5.0)
    swirl = 0.0
    rough = jnp.exp(jax.random.uniform(keys[1], shape, jnp.float32, -0.45, 0.45))
    phase = jax.random.uniform(keys[2], (3, 1, 1, 1), jnp.float32, 0.0, 2.0 * math.pi)
    wave = jnp.cos(2.0 * math.pi * (3.0 * theta_pos + 2.0 * axial_pos) + phase) * jnp.sin(math.pi * radius)
    amplitude = 0.02 * (1.0 + 2.0 * theta_pos) * (1.0 + 2.0 * axial_pos) * radius
    fluctuation = amplitude * (noise * rough + 2.0 * theta_pos * wave)
    ones = jnp.ones((1, NTH, NZ, NR), jnp.float32)
    mean = jnp.concatenate([0.0 * ones, swirl * radius * ones, (1.0 - radius ** 2) * ones], axis=0)
    return fluctuation + mean


def setup_inputs(seed: int = 0) -> dict:
    key_list = jax.random.split(jax.random.key(seed), 2)
    return {
        "velocity": draw_velocity(jax.random.fold_in(key_list[1], 71), 0),
    }


pipe_length = 4.0 * math.pi
nu_molecular = 5e-05
time_step = 2.0
filter_ratio = 4.0
epsilon_den = 1e-06
pair_first = (0, 1, 2, 0, 0, 1)
pair_second = (0, 1, 2, 1, 2, 2)

def grid_terms():
    radial_step = 1.0 / NR
    radius = (jnp.arange(NR, dtype=jnp.float32) + 0.5) * radial_step
    theta_step = 2.0 * math.pi / NTH
    axial_step = pipe_length / NZ
    width_sq = jnp.cbrt(radial_step * radius * theta_step * axial_step) ** 2
    return (radius, width_sq)

def along_theta(padded):
    return (padded[..., 2:, 1:-1, :] - padded[..., :-2, 1:-1, :]) * (0.5 * NTH / (2.0 * math.pi))

def along_axis(padded):
    return (padded[..., 1:-1, 2:, :] - padded[..., 1:-1, :-2, :]) * (0.5 * NZ / pipe_length)

def along_radius(field):
    zeros = jnp.zeros(field.shape[:-1] + (1,), field.dtype)
    extended = jnp.concatenate([zeros, field, zeros], axis=-1)
    return (extended[..., 2:] - extended[..., :-2]) * (0.5 * NR)

def interior(padded):
    return padded[..., 1:-1, 1:-1, :]

def strain(padded, radius):
    centre = interior(padded)
    radial = along_radius(centre)
    azimuthal = along_theta(padded) / radius
    axial = along_axis(padded)
    return jnp.stack([radial[0], azimuthal[1] + centre[0] / radius, axial[2], 0.5 * (radial[1] - centre[1] / radius + azimuthal[0]), 0.5 * (axial[0] + radial[2]), 0.5 * (azimuthal[2] + axial[1])])

def magnitude(tensor):
    return jnp.sqrt(2.0 * (tensor[0] ** 2 + tensor[1] ** 2 + tensor[2] ** 2) + 4.0 * (tensor[3] ** 2 + tensor[4] ** 2 + tensor[5] ** 2))

def test_filter(padded):
    across = 0.25 * padded[..., :-2, :, :] + 0.5 * padded[..., 1:-1, :, :] + 0.25 * padded[..., 2:, :, :]
    return 0.25 * across[..., :, :-2, :] + 0.5 * across[..., :, 1:-1, :] + 0.25 * across[..., :, 2:, :]

def products(flow, tensor):
    pairs = jnp.stack([flow[first_comp] * flow[second_comp] for first_comp, second_comp in zip(pair_first, pair_second)])
    return jnp.concatenate([flow, pairs, tensor, magnitude(tensor) * tensor], axis=0)

def germano(filtered, width_sq):
    means = filtered[0:3]
    pairs = jnp.stack([means[first_comp] * means[second_comp] for first_comp, second_comp in zip(pair_first, pair_second)])
    leonard = filtered[3:9] - pairs
    smooth = filtered[9:15]
    model = 2.0 * width_sq * (filter_ratio * magnitude(smooth) * smooth - filtered[15:21])
    weights = jnp.array([1.0, 1.0, 1.0, 2.0, 2.0, 2.0], dtype=jnp.float32)[:, None, None, None]
    return (lax.optimization_barrier(jnp.sum(weights * leonard * model, axis=(0, 1, 2))), lax.optimization_barrier(jnp.sum(weights * model * model, axis=(0, 1, 2))))

def divergence(stress, radius):
    centre = interior(stress)
    radial = along_radius(centre)
    azimuthal = along_theta(stress) / radius
    axial = along_axis(stress)
    return jnp.stack([radial[0] + azimuthal[3] + axial[4] + (centre[0] - centre[1]) / radius, radial[3] + azimuthal[1] + axial[5] + 2.0 * centre[3] / radius, radial[4] + azimuthal[5] + axial[2] + centre[4] / radius])

def continuity(padded, radius):
    centre = interior(padded)
    return along_radius(radius * centre[0]) / radius + along_theta(padded[1]) / radius + along_axis(padded[2])

def mode_solve(real_part, imag_part, theta_modes, axial_modes, radius):
    radial_step = 1.0 / NR
    lower = (radius - 0.5 * radial_step) / radius * (NR * NR)
    upper = (radius + 0.5 * radial_step) / radius * (NR * NR)
    last = jnp.arange(NR, dtype=jnp.int32) == NR - 1
    centre = -(lower + upper) - jnp.where(last, upper, 0.0)
    upper = jnp.where(last, 0.0, upper)
    theta_wave = jnp.minimum(theta_modes, NTH - theta_modes).astype(jnp.float32)
    axial_wave = jnp.minimum(axial_modes, NZ - axial_modes).astype(jnp.float32) * (2.0 * math.pi / pipe_length)
    diagonal = centre - (theta_wave[:, None, None] / radius) ** 2 - axial_wave[None, :, None] ** 2
    shape = diagonal.shape
    solved = lax.linalg.tridiagonal_solve(jnp.broadcast_to(lower, shape), diagonal, jnp.broadcast_to(upper, shape), jnp.stack([real_part, imag_part], axis=-1))
    return jnp.moveaxis(solved, -1, 0)

def reference(velocity):
    radius, width_sq = grid_terms()
    slab_count = 8
    slab_len = NZ // slab_count
    padded = jnp.pad(velocity, ((0, 0), (3, 3), (3, 3), (0, 0)), mode='wrap')
    starts = jnp.arange(slab_count, dtype=jnp.int32) * slab_len

    def shell_terms(start):
        piece = lax.dynamic_slice_in_dim(padded, start + 1, slab_len + 4, axis=2)[:, 1:-1]
        tensor = strain(piece, radius)
        filtered = test_filter(products(interior(piece), tensor))
        return germano(filtered, width_sq)
    numer, denom = lax.map(shell_terms, starts)
    coefficient = lax.optimization_barrier(jnp.sum(numer, axis=0)) / (lax.optimization_barrier(jnp.sum(denom, axis=0)) + epsilon_den)

    def source_terms(start):
        piece = lax.dynamic_slice_in_dim(padded, start, slab_len + 6, axis=2)
        tensor = strain(piece, radius)
        eddy = coefficient * width_sq * magnitude(tensor)
        stress = 2.0 * (nu_molecular + eddy) * tensor
        star = interior(interior(piece)) + time_step * divergence(stress, radius)
        return (continuity(star, radius), interior(interior(eddy)) / nu_molecular)
    sources, ratios = lax.map(source_terms, starts)
    source = jnp.moveaxis(sources, 0, 1).reshape(NTH, NZ, NR)
    ratio = jnp.moveaxis(ratios, 0, 1).reshape(NTH, NZ, NR)
    spectrum = jnp.fft.fft2(source, axes=(0, 1)) / math.sqrt(NTH * NZ)
    pressure = mode_solve(jnp.real(spectrum).astype(jnp.float32), jnp.imag(spectrum).astype(jnp.float32), jnp.arange(NTH, dtype=jnp.int32), jnp.arange(NZ, dtype=jnp.int32), radius)
    return (ratio, pressure)
```

```python
import functools
import math

import jax
import jax.numpy as jnp
import numpy as np
from jax import lax
from jax.experimental import pallas as pl
from jax.experimental.pallas import tpu as pltpu
from jax.sharding import PartitionSpec as P

pipe_length = 4.0 * math.pi
nu_molecular = 5e-05
time_step = 2.0
filter_ratio = 4.0
epsilon_den = 1e-06
CHUNKS = 2
VMEM_BYTES = 60 * 1024 * 1024
ANY = pl.BlockSpec(memory_space=pl.ANY)
VM = pl.BlockSpec(memory_space=pltpu.VMEM)


def params(limit=VMEM_BYTES):
    return pltpu.CompilerParams(vmem_limit_bytes=limit)


def round_up(value, unit):
    return (value + unit - 1) // unit * unit


class Grid:
    def __init__(self, velocity):
        self.nt = lax.axis_size("theta")
        self.ng = lax.axis_size("gz")
        _, self.T, self.Z, self.R = velocity.shape
        self.NTH = self.T * self.nt
        self.NZ = self.Z * self.ng
        self.kb = self.NZ // self.nt
        self.mb = self.NTH // self.ng
        self.chunks = CHUNKS
        while self.R % (self.chunks * self.ng):
            self.chunks //= 2
        self.rc = self.R // self.chunks
        self.rb = self.rc // self.ng
        self.kz = 0.5 * self.NZ / pipe_length
        self.kt = 0.5 * self.NTH / (2.0 * math.pi)

    def lanes(self):
        R = self.R
        index = lax.broadcasted_iota(jnp.int32, (8, R), 1)
        radius = (index.astype(jnp.float32) + 0.5) * (1.0 / R)
        inverse = 1.0 / radius
        up = jnp.where(index == R - 1, 0.0, 0.5 * R)
        down = jnp.where(index == 0, 0.0, 0.5 * R)
        return radius, inverse, up, down


def width_row(g):
    radius = (np.arange(g.R, dtype=np.float32) + np.float32(0.5)) * np.float32(1.0 / g.R)
    cell = radius.astype(np.float64) * (1.0 / g.R) * (2.0 * math.pi / g.NTH) * (pipe_length / g.NZ)
    return jnp.asarray(np.broadcast_to((np.cbrt(cell) ** 2).astype(np.float32), (8, g.R)))


def shift_up(f):
    return pltpu.roll(f, f.shape[-1] - 1, 1)


def shift_down(f):
    return pltpu.roll(f, 1, 1)


def strain_rows(pad, t, z, g, rows):
    inverse, up, down, kt = rows
    at = lambda c, dt, dz: pad[c, t + dt, z + dz : z + dz + 8, :]
    u = [at(c, 0, 0) for c in range(3)]
    radial = [shift_up(f) * up - shift_down(f) * down for f in u]
    turn = [(at(c, 1, 0) - at(c, -1, 0)) * kt for c in range(3)]
    axial = [(at(c, 0, 1) - at(c, 0, -1)) * g.kz for c in range(3)]
    ur, ut = u[0] * inverse, u[1] * inverse
    s = [
        radial[0],
        turn[1] + ur,
        axial[2],
        radial[1] - ut + turn[0],
        axial[0] + radial[2],
        turn[2] + axial[1],
    ]
    return u, s


def root(x):
    return x * lax.rsqrt(jnp.maximum(x, 1e-36))


def size_of(s):
    diag = s[0] * s[0] + s[1] * s[1] + s[2] * s[2]
    return root((diag + diag) + (s[3] * s[3] + s[4] * s[4] + s[5] * s[5]))


def fill_pad(g, v, tlo, thi, zlo, zhi, pad, sems):
    T, Z = g.T, g.Z
    copies = [
        pltpu.make_async_copy(v, pad.at[:, pl.ds(3, T), pl.ds(8, Z), :], sems.at[0]),
        pltpu.make_async_copy(tlo, pad.at[:, pl.ds(0, 3), pl.ds(8, Z), :], sems.at[1]),
        pltpu.make_async_copy(thi, pad.at[:, pl.ds(T + 3, 3), pl.ds(8, Z), :], sems.at[2]),
    ]
    for copy in copies:
        copy.start()
    rows = pad.reshape(3 * (T + 6) * (Z + 16), g.R)
    for c in range(3):
        for i in range(3):
            first = c * (T + 6) * (Z + 16)
            rows[pl.ds(first + 5 + i, T + 6, stride=Z + 16), :] = zlo[c, i]
            rows[pl.ds(first + 8 + Z + i, T + 6, stride=Z + 16), :] = zhi[c, i]
    for copy in copies:
        copy.wait()


PAIRS = ((0, 0), (1, 1), (2, 2), (0, 1), (0, 2), (1, 2))


def sums_kernel(g, v, tlo, thi, zlo, zhi, width, out, pad, raw, last, pair, acc, sems):
    fill_pad(g, v, tlo, thi, zlo, zhi, pad, sems)
    _, inverse, up, down = g.lanes()
    rows = (inverse, up, down, g.kt * inverse)
    acc[...] = jnp.zeros_like(acc)

    def step(t, carry):
        for zc in range(raw.shape[1] // 8):
            z = 7 + 8 * zc
            u, s = strain_rows(pad, t + 2, z, g, rows)
            size = size_of(s)
            here = pl.ds(8 * zc, 8)
            for n, (a, b) in enumerate(PAIRS):
                raw[n, here, :] = u[a] * u[b]
                raw[6 + n, here, :] = s[n]
                raw[12 + n, here, :] = size * s[n]
        live = t >= 2

        def smooth(n, load, zc):
            centre = load(1)
            h = (load(0) + load(2)) + (centre + centre)
            here = pl.ds(8 * zc, 8)
            two = last[n, here, :] + h
            result = pair[n, here, :] + two
            last[n, here, :] = h
            pair[n, here, :] = two
            return result

        for zc in range(g.Z // 8):
            mean = [
                smooth(c, lambda d, c=c: pad[c, t + 2, 7 + 8 * zc + d : 15 + 8 * zc + d, :], zc)
                for c in range(3)
            ]
            field = lambda n: smooth(
                3 + n, lambda d: raw[n, 8 * zc + d : 8 * zc + d + 8, :], zc
            )
            scaled = [m * 0.0625 for m in mean]
            leonard = [field(n) - scaled[a] * mean[b] for n, (a, b) in enumerate(PAIRS)]
            calm = [field(6 + n) for n in range(6)]
            size = size_of(calm) * (filter_ratio / 16.0)
            model = [size * calm[n] - field(12 + n) for n in range(6)]
            numer = leonard[0] * model[0]
            for n in range(1, 6):
                numer = numer + leonard[n] * model[n]
            diag = model[0] * model[0] + model[1] * model[1] + model[2] * model[2]
            side = model[3] * model[3] + model[4] * model[4] + model[5] * model[5]
            acc[0] += jnp.where(live, numer, 0.0)
            acc[1] += jnp.where(live, diag + 0.5 * side, 0.0)
        return carry

    lax.fori_loop(0, g.T + 2, step, 0)
    w = width[...] * (2.0 / 16.0)
    numer = jnp.sum(acc[0], axis=0, keepdims=True) * (w[:1] * (1.0 / 16.0))
    denom = jnp.sum(acc[1], axis=0, keepdims=True) * (w[:1] * w[:1])
    index = lax.broadcasted_iota(jnp.int32, (8, g.R), 0)
    out[...] = jnp.where(index == 0, numer, jnp.where(index == 1, denom, 0.0))


def source_kernel(g, v, tlo, thi, zlo, zhi, width, sums, ratio, *rest):
    outs = rest[: g.chunks * g.ng]
    pad, tau, eddy, vt, vz, src, flip, sems, osems = rest[g.chunks * g.ng :]
    T, Z, R = g.T, g.Z, g.R
    fill_pad(g, v, tlo, thi, zlo, zhi, pad, sems)
    radius, inverse, up, down = g.lanes()
    rows = (inverse, up, down, g.kt * inverse)
    kt = rows[3]
    total = jnp.sum(sums[...], axis=0)
    coefficient = total[0:1] / (total[1:2] + epsilon_den)
    strength = jnp.broadcast_to(coefficient, (8, R)) * width[...]

    def stress_row(t, carry):
        for zc in range(eddy.shape[1] // 8):
            z = 6 + 8 * zc
            _, s = strain_rows(pad, t + 1, z, g, rows)
            e = strength * size_of(s)
            here = pl.ds(8 * zc, 8)
            eddy[t, here, :] = e * (1.0 / nu_molecular)
            side = time_step * (nu_molecular + e)
            main = side + side
            for n in range(3):
                tau[n, t, here, :] = main * s[n]
                tau[3 + n, t, here, :] = side * s[3 + n]
        return carry

    lax.fori_loop(0, T + 4, stress_row, 0)

    def slab(n, t, z):
        return tau[n, t, z : z + 8, :]

    def radial(f):
        return shift_up(f) * up - shift_down(f) * down

    def turn_row(a, carry):
        t = a + 1
        for zc in range(Z // 8):
            z = 2 + 8 * zc
            rt = slab(3, t, z)
            force = (
                radial(rt)
                + (slab(1, t + 1, z) - slab(1, t - 1, z)) * kt
                + (slab(5, t, z + 1) - slab(5, t, z - 1)) * g.kz
                + rt * (inverse + inverse)
            )
            vt[a, pl.ds(8 * zc, 8), :] = pad[1, a + 2, 8 + 8 * zc : 16 + 8 * zc, :] + force
        return carry

    lax.fori_loop(0, T + 2, turn_row, 0)
    r_up = shift_up(radius) * inverse * up
    r_down = shift_down(radius) * inverse * down

    def source_row(a, carry):
        t = a + 2
        for zc in range(vz.shape[0] // 8):
            z = 1 + 8 * zc
            rz = slab(4, t, z)
            force = (
                radial(rz)
                + (slab(5, t + 1, z) - slab(5, t - 1, z)) * kt
                + (slab(2, t, z + 1) - slab(2, t, z - 1)) * g.kz
                + rz * inverse
            )
            vz[pl.ds(8 * zc, 8), :] = pad[2, a + 3, 7 + 8 * zc : 15 + 8 * zc, :] + force
        for zc in range(Z // 8):
            z = 2 + 8 * zc
            here = pl.ds(8 * zc, 8)
            rr = slab(0, t, z)
            force = (
                radial(rr)
                + (slab(3, t + 1, z) - slab(3, t - 1, z)) * kt
                + (slab(4, t, z + 1) - slab(4, t, z - 1)) * g.kz
                + (rr - slab(1, t, z)) * inverse
            )
            vr = pad[0, a + 3, 8 + 8 * zc : 16 + 8 * zc, :] + force
            src[a, here, :] = (
                shift_up(vr) * r_up
                - shift_down(vr) * r_down
                + (vt[a + 2, here, :] - vt[a, here, :]) * kt
                + (vz[8 * zc + 2 : 8 * zc + 10, :] - vz[8 * zc : 8 * zc + 8, :]) * g.kz
            )
            ratio[a, here, :] = eddy[t, z : z + 8, :]
        return carry

    lax.fori_loop(0, T, source_row, 0)
    flat = src.reshape(T * src.shape[1], R)
    turned = flip.reshape(R * flip.shape[1], 2 * T)

    def flip_step(p, carry):
        even = flat[pl.ds(2 * p, T, stride=src.shape[1]), :]
        odd = flat[pl.ds(2 * p + 1, T, stride=src.shape[1]), :]
        turned[pl.ds(p, R, stride=flip.shape[1]), :] = jnp.concatenate([even, odd], axis=0).T
        return carry

    lax.fori_loop(0, Z // 2, flip_step, 0)
    me = lax.axis_index("gz")
    copies = []
    for c in range(g.chunks):
        for s in range(g.ng):
            first = c * g.rc + lax.rem(me + s, g.ng) * g.rb
            n = c * g.ng + s
            copies.append(
                pltpu.make_async_copy(
                    flip.at[pl.ds(first, g.rb), pl.ds(0, Z // 2), :], outs[n], osems.at[n]
                )
            )
    for copy in copies:
        copy.start()
    for copy in copies:
        copy.wait()


def split(x):
    parts = []
    for _ in range(2):
        parts.append(x.astype(jnp.bfloat16))
        x = x - parts[-1].astype(jnp.float32)
    return parts + [x.astype(jnp.bfloat16)]


def split_table(x):
    parts = []
    for _ in range(2):
        high = lax.reduce_precision(x, 8, 7)
        parts.append(high.astype(jnp.bfloat16))
        x = x - high
    return parts + [x.astype(jnp.bfloat16)]


def dot6(a, b):
    dot = functools.partial(jnp.dot, preferred_element_type=jnp.float32)
    small = dot(a[1], b[1]) + dot(a[2], b[0]) + dot(a[0], b[2])
    return dot(a[0], b[0]) + (dot(a[1], b[0]) + dot(a[0], b[1]) + small)


def axial_kernel(g, *refs):
    blocks, tables = refs[: g.ng], refs[g.ng : g.ng + 3]
    outs = refs[g.ng + 3 : g.ng + 3 + g.nt]
    left = refs[g.ng + 3 + g.nt :]
    T, zp, kb = g.T, g.Z // 2, g.kb
    mine, other = lax.axis_index("gz"), lax.axis_index("theta")
    for s in range(g.ng):
        source = lax.rem(mine + g.ng - s, g.ng)
        for d in range(g.nt):
            target = lax.rem(other + d, g.nt)
            here = (pl.ds(d * kb, kb), pl.ds(4 * zp * s, 4 * zp))
            for n in range(3):
                left[n][here] = tables[n][source, target]
    per = 2 if g.rb % 2 == 0 else 1
    first = lax.broadcasted_iota(jnp.int32, (zp, 2 * T), 1) < T

    def column(r):
        parts = []
        for s in range(g.ng):
            x = blocks[s][r]
            y = jnp.concatenate([x[:, T:], x[:, :T]], axis=1)
            for f in (x, y):
                parts.append(jnp.where(first, f, 0.0))
                parts.append(jnp.where(first, 0.0, f))
        return jnp.concatenate(parts, axis=0)

    def step(i, carry):
        right = jnp.concatenate([column(per * i + q) for q in range(per)], axis=1)
        result = dot6([w[...] for w in left], split(right))
        for q in range(per):
            for d in range(g.nt):
                outs[d][per * i + q] = result[d * kb : (d + 1) * kb, q * 2 * T : (q + 1) * 2 * T]
        return carry

    lax.fori_loop(0, g.rb // per, step, 0)


def turn_kernel(g, *refs):
    blocks, tables = refs[: g.nt], refs[g.nt : g.nt + 3]
    outs = refs[g.nt + 3 : g.nt + 3 + g.ng]
    mine, other = lax.axis_index("theta"), lax.axis_index("gz")
    rows = g.rb * g.kb
    left = split(jnp.concatenate([b[...].reshape(rows, 2 * g.T) for b in blocks], axis=1))
    for d in range(g.ng):
        target = lax.rem(other + d, g.ng)
        source = [lax.rem(mine + g.nt - s, g.nt) for s in range(g.nt)]
        right = [jnp.concatenate([w[target, s] for s in source], axis=0) for w in tables]
        result = dot6(left, right)
        for c in range(2):
            part = result[:, c * g.mb : (c + 1) * g.mb]
            outs[d][c] = part.reshape(g.rb, g.kb, g.mb)


def solve_kernel(g, *refs):
    count = g.chunks * g.ng
    blocks, coefs, out = refs[:count], refs[count], refs[count + 1]
    data, factor, flip, sems, osems = refs[count + 2 :]
    R, kb, mb = g.R, g.kb, g.mb
    mine, other = lax.axis_index("gz"), lax.axis_index("theta")
    copies = []
    for c in range(g.chunks):
        for s in range(g.ng):
            first = c * g.rc + lax.rem(mine + g.ng - s, g.ng) * g.rb
            n = c * g.ng + s
            copies.append(
                pltpu.make_async_copy(
                    blocks[n], data.at[:, pl.ds(first, g.rb), pl.ds(0, kb), :], sems.at[n]
                )
            )
    for copy in copies:
        copy.start()
    for copy in copies:
        copy.wait()
    m = mine * mb + lax.broadcasted_iota(jnp.int32, (kb, mb), 1)
    k = other * kb + lax.broadcasted_iota(jnp.int32, (kb, mb), 0)
    a = jnp.minimum(m, g.NTH - m).astype(jnp.float32)
    q = jnp.minimum(k, g.NZ - k).astype(jnp.float32) * (2.0 * math.pi / pipe_length)
    a2, q2 = a * a, q * q
    zero = jnp.zeros((kb, mb), jnp.float32)

    def forward(r, carry):
        cp, re, im = carry
        lower, upper, centre, inv2 = (coefs[n, r] for n in range(4))
        w = 1.0 / ((centre - q2) - a2 * inv2 - lower * cp)
        cp = upper * w
        re = (data[0, r, :kb, :] - lower * re) * w
        im = (data[1, r, :kb, :] - lower * im) * w
        factor[r] = cp
        data[0, r, :kb, :] = re
        data[1, r, :kb, :] = im
        return cp, re, im

    lax.fori_loop(0, R, forward, (zero, zero, zero), unroll=2)

    def backward(i, carry):
        re, im = carry
        r = R - 1 - i
        cp = factor[r]
        re = data[0, r, :kb, :] - cp * re
        im = data[1, r, :kb, :] - cp * im
        data[0, r, :kb, :] = re
        data[1, r, :kb, :] = im
        return re, im

    lax.fori_loop(0, R, backward, (zero, zero), unroll=2)
    flat = data.reshape(2 * R * data.shape[2], mb)
    turned = flip.reshape(2 * mb * flip.shape[2], R)
    stores = []
    for c in range(2):

        def flip_step(i, carry):
            rows = flat[pl.ds(c * R * data.shape[2] + i, R, stride=data.shape[2]), :]
            turned[pl.ds(c * mb * flip.shape[2] + i, mb, stride=flip.shape[2]), :] = rows.T
            return carry

        lax.fori_loop(0, kb, flip_step, 0)
        copy = pltpu.make_async_copy(flip.at[c, :, pl.ds(0, kb), :], out.at[c], osems.at[c])
        copy.start()
        stores.append(copy)
    for copy in stores:
        copy.wait()


def exchange(blocks, axis):
    count = len(blocks)
    return [blocks[0]] + [
        lax.ppermute(blocks[s], axis, [(i, (i + s) % count) for i in range(count)])
        for s in range(1, count)
    ]


def halo(g, v):
    T, Z = g.T, g.Z

    def pair(low, high, axis, count):
        forward = [(i, (i + 1) % count) for i in range(count)]
        backward = [(target, source) for source, target in forward]
        return lax.ppermute(high, axis, forward), lax.ppermute(low, axis, backward)

    tlo, thi = pair(v[:, :3], v[:, T - 3 :], "theta", g.nt)
    face = lambda first: jnp.concatenate(
        [f[:, :, first : first + 3].transpose(0, 2, 1, 3) for f in (tlo, v, thi)], axis=2
    )
    zlo, zhi = pair(face(0), face(Z - 3), "gz", g.ng)
    return tlo, thi, zlo, zhi


def axial_table(g):
    z, k = np.arange(g.NZ), np.arange(g.NZ)
    angle = 2.0 * math.pi * ((k[:, None] * z[None, :]) % g.NZ) / g.NZ
    scale = 1.0 / math.sqrt(g.NTH * g.NZ)
    cos = (np.cos(angle) * scale).reshape(g.nt, g.kb, g.ng, g.Z // 2, 2)
    sin = (-np.sin(angle) * scale).reshape(g.nt, g.kb, g.ng, g.Z // 2, 2)
    parts = [cos[..., 0], sin[..., 1], cos[..., 1], sin[..., 0]]
    table = np.stack(parts, axis=3).reshape(g.nt, g.kb, g.ng, 2 * g.Z)
    return split_table(jnp.asarray(table.transpose(2, 0, 1, 3).astype(np.float32)))


def turn_table(g):
    t, m = np.arange(g.T), np.arange(g.NTH)
    base = 2.0 * math.pi * ((t[:, None] * m[None, :]) % g.NTH) / g.NTH
    skip = 2.0 * math.pi * ((np.arange(g.nt)[:, None] * g.T * m[None, :]) % g.NTH) / g.NTH
    f32 = lambda x: jnp.asarray(x.astype(np.float32))
    fold = lambda x: x.reshape(x.shape[0], g.ng, g.mb).transpose(1, 0, 2)
    c0, s0 = f32(fold(np.cos(base)))[:, None], f32(fold(np.sin(base)))[:, None]
    c1, s1 = f32(fold(np.cos(skip)))[:, :, None], f32(fold(np.sin(skip)))[:, :, None]
    cos = c0 * c1 - s0 * s1
    sin = s0 * c1 + c0 * s1
    top = jnp.concatenate([cos, -sin], axis=-1)
    bottom = jnp.concatenate([sin, cos], axis=-1)
    return split_table(jnp.concatenate([top, bottom], axis=-2))


def solve_coefs(g):
    R = g.R
    radius = (np.arange(R) + 0.5) / R
    lower = (radius - 0.5 / R) / radius * (R * R)
    upper = (radius + 0.5 / R) / radius * (R * R)
    last = np.arange(R) == R - 1
    centre = -(lower + upper) - np.where(last, upper, 0.0)
    upper = np.where(last, 0.0, upper)
    return jnp.asarray(np.stack([lower, upper, centre, 1.0 / radius**2]).astype(np.float32))


def body(velocity):
    g = Grid(velocity)
    T, Z, R, rb, kb, mb = g.T, g.Z, g.R, g.rb, g.kb, g.mb
    f32 = jnp.float32
    shape = lambda *s: jax.ShapeDtypeStruct(s, f32)
    buf = lambda *s: pltpu.VMEM(s, f32)
    dma = pltpu.SemaphoreType.DMA
    edges = halo(g, velocity)
    width = width_row(g)
    pad = buf(3, T + 6, Z + 16, R)
    halo_specs = [ANY, ANY, ANY, VM, VM, VM]
    part = pl.pallas_call(
        functools.partial(sums_kernel, g),
        out_shape=shape(8, R),
        in_specs=halo_specs,
        out_specs=VM,
        scratch_shapes=[
            pad,
            buf(18, round_up(Z + 2, 8), R),
            buf(21, Z, R),
            buf(21, Z, R),
            buf(2, 8, R),
            dma((3,)),
        ],
        compiler_params=params(),
        name="germano_sums",
    )(velocity, *edges, width)
    count = g.nt * g.ng
    sums = lax.all_to_all(
        jnp.broadcast_to(part[None], (count, 8, R)), ("theta", "gz"), 0, 0, tiled=True
    )
    outs = pl.pallas_call(
        functools.partial(source_kernel, g),
        out_shape=[shape(T, Z, R)] + [shape(rb, Z // 2, 2 * T)] * (g.chunks * g.ng),
        in_specs=halo_specs + [VM],
        out_specs=[VM] + [ANY] * (g.chunks * g.ng),
        scratch_shapes=[
            pad,
            buf(6, T + 4, round_up(Z + 4, 8) + 8, R),
            buf(T + 4, round_up(Z + 4, 8), R),
            buf(T + 2, Z, R),
            buf(round_up(Z + 2, 8), R),
            buf(T, Z + 8, R),
            buf(R, Z // 2 + 8, 2 * T),
            dma((3,)),
            dma((g.chunks * g.ng,)),
        ],
        compiler_params=params(),
        name="source",
    )(velocity, *edges, width, sums)
    ratio, pieces = outs[0], outs[1:]
    axial_tables = axial_table(g)
    turn_tables = turn_table(g)
    modes = []
    for c in range(g.chunks):
        lines = exchange(pieces[c * g.ng : (c + 1) * g.ng], "gz")
        axial = pl.pallas_call(
            functools.partial(axial_kernel, g),
            out_shape=[shape(rb, kb, 2 * T)] * g.nt,
            in_specs=[VM] * (g.ng + 3),
            out_specs=[VM] * g.nt,
            scratch_shapes=[pltpu.VMEM((g.NZ, 2 * g.NZ), jnp.bfloat16)] * 3,
            compiler_params=params(24 * 1024 * 1024),
            name="axial_modes",
        )(*lines, *axial_tables)
        cycles = exchange(axial, "theta")
        turned = pl.pallas_call(
            functools.partial(turn_kernel, g),
            out_shape=[shape(2, rb, kb, mb)] * g.ng,
            in_specs=[VM] * (g.nt + 3),
            out_specs=[VM] * g.ng,
            compiler_params=params(40 * 1024 * 1024),
            name="turn_modes",
        )(*cycles, *turn_tables)
        modes += exchange(turned, "gz")
    pressure = pl.pallas_call(
        functools.partial(solve_kernel, g),
        out_shape=shape(2, mb, kb, R),
        in_specs=[ANY] * len(modes) + [pl.BlockSpec(memory_space=pltpu.SMEM)],
        out_specs=ANY,
        scratch_shapes=[
            buf(2, R, kb + 8, mb),
            buf(R, kb, mb),
            buf(2, mb, kb + 8, R),
            dma((len(modes),)),
            dma((2,)),
        ],
        compiler_params=params(40 * 1024 * 1024),
        name="solve_modes",
    )(*modes, solve_coefs(g))
    return (ratio, pressure)


def solution(mesh):
    return jax.shard_map(
        body,
        mesh=mesh,
        in_specs=(P(None, "theta", "gz", None),),
        out_specs=(P("theta", "gz", None), P(None, "gz", "theta", None)),
        check_vma=False,
    )
```

```python
import functools
import math

import jax
import jax.numpy as jnp
import numpy as np
from jax import lax
from jax.experimental import pallas as pl
from jax.experimental.pallas import tpu as pltpu
from jax.sharding import PartitionSpec as P

pipe_length = 4.0 * math.pi
nu_molecular = 5e-05
time_step = 2.0
filter_ratio = 4.0
epsilon_den = 1e-06
CHUNK_EDGES = (0, 6, 16, 26, 32)
UNROLL_SUMS = 1
UNROLL = 4
VMEM_BYTES = 60 * 1024 * 1024
ANY = pl.BlockSpec(memory_space=pl.ANY)
VM = pl.BlockSpec(memory_space=pltpu.VMEM)


def params(limit=VMEM_BYTES):
    return pltpu.CompilerParams(vmem_limit_bytes=limit)


def round_up(value, unit):
    return (value + unit - 1) // unit * unit


def odd_tiles(rows):
    return (round_up(rows, 8) // 8 | 1) * 8


def loop(count, most, step):
    unit = next(u for u in range(most, 0, -1) if count % u == 0)

    def several(i, carry):
        for slot in range(unit):
            step(i * unit + slot, slot)
        return carry

    lax.fori_loop(0, count // unit, several, 0)


class Grid:
    def __init__(self, velocity):
        self.nt = lax.axis_size("theta")
        self.ng = lax.axis_size("gz")
        _, self.T, self.Z, self.R = velocity.shape
        self.chunks = len(CHUNK_EDGES) - 1
        self.NTH = self.T * self.nt
        self.NZ = self.Z * self.ng
        self.kb = self.NZ // self.nt
        self.mb = self.NTH // self.ng
        share = self.R // self.ng
        edges = [round(share * e / 32.0 / 2) * 2 for e in CHUNK_EDGES]
        self.first = edges[:-1]
        self.rb = [b - a for a, b in zip(edges, edges[1:])]
        self.kz = 0.5 * self.NZ / pipe_length
        self.kt = 0.5 * self.NTH / (2.0 * math.pi)

    def lanes(self):
        R = self.R
        index = lax.broadcasted_iota(jnp.int32, (8, R), 1)
        radius = (index.astype(jnp.float32) + 0.5) * (1.0 / R)
        inverse = 1.0 / radius
        up = jnp.where(index == R - 1, 0.0, 0.5 * R)
        down = jnp.where(index == 0, 0.0, 0.5 * R)
        return radius, inverse, up, down


def width_row(g):
    radius = (np.arange(g.R, dtype=np.float32) + np.float32(0.5)) * np.float32(1.0 / g.R)
    cell = radius.astype(np.float64) * (1.0 / g.R) * (2.0 * math.pi / g.NTH) * (pipe_length / g.NZ)
    return jnp.asarray(np.broadcast_to((np.cbrt(cell) ** 2).astype(np.float32), (8, g.R)))


def shift_up(f):
    return pltpu.roll(f, f.shape[-1] - 1, 1)


def shift_down(f):
    return pltpu.roll(f, 1, 1)


def strain_rows(pad, t, z, g, rows):
    inverse, up, down, kt = rows
    at = lambda c, dt, dz: pad[c, t + dt, z + dz : z + dz + 8, :]
    u = [at(c, 0, 0) for c in range(3)]
    radial = [shift_up(f) * up - shift_down(f) * down for f in u]
    turn = [(at(c, 1, 0) - at(c, -1, 0)) * kt for c in range(3)]
    axial = [(at(c, 0, 1) - at(c, 0, -1)) * g.kz for c in range(3)]
    ur, ut = u[0] * inverse, u[1] * inverse
    s = [
        radial[0],
        turn[1] + ur,
        axial[2],
        radial[1] - ut + turn[0],
        axial[0] + radial[2],
        turn[2] + axial[1],
    ]
    return u, s


def root(x):
    return x * lax.rsqrt(jnp.maximum(x, 1e-36))


def size_of(s):
    diag = s[0] * s[0] + s[1] * s[1] + s[2] * s[2]
    return root((diag + diag) + (s[3] * s[3] + s[4] * s[4] + s[5] * s[5]))


def fill_pad(g, v, tlo, thi, zlo, zhi, pad, sems):
    T, Z = g.T, g.Z
    copies = [
        pltpu.make_async_copy(v, pad.at[:, pl.ds(3, T), pl.ds(8, Z), :], sems.at[0]),
        pltpu.make_async_copy(tlo, pad.at[:, pl.ds(0, 3), pl.ds(8, Z), :], sems.at[1]),
        pltpu.make_async_copy(thi, pad.at[:, pl.ds(T + 3, 3), pl.ds(8, Z), :], sems.at[2]),
    ]
    for copy in copies:
        copy.start()
    pitch = pad.shape[2]
    rows = pad.reshape(3 * (T + 6) * pitch, g.R)
    for c in range(3):
        for i in range(3):
            first = c * (T + 6) * pitch
            rows[pl.ds(first + 5 + i, T + 6, stride=pitch), :] = zlo[c, i]
            rows[pl.ds(first + 8 + Z + i, T + 6, stride=pitch), :] = zhi[c, i]
    for copy in copies:
        copy.wait()


PAIRS = ((0, 0), (1, 1), (2, 2), (0, 1), (0, 2), (1, 2))


def sums_kernel(g, v, tlo, thi, zlo, zhi, width, out, pad, raw, last, pair, acc, sems):
    fill_pad(g, v, tlo, thi, zlo, zhi, pad, sems)
    _, inverse, up, down = g.lanes()
    rows = (inverse, up, down, g.kt * inverse)
    acc[...] = jnp.zeros_like(acc)

    def step(t, slot):
        for zc in range(round_up(g.Z + 2, 8) // 8):
            z = 7 + 8 * zc
            u, s = strain_rows(pad, t + 2, z, g, rows)
            size = size_of(s)
            here = pl.ds(8 * zc, 8)
            for n, (a, b) in enumerate(PAIRS):
                raw[slot, n, here, :] = u[a] * u[b]
                raw[slot, 6 + n, here, :] = s[n]
                raw[slot, 12 + n, here, :] = size * s[n]
        live = t >= 2

        def smooth(n, load, zc):
            centre = load(1)
            h = (load(0) + load(2)) + (centre + centre)
            here = pl.ds(8 * zc, 8)
            two = last[n, here, :] + h
            result = pair[n, here, :] + two
            last[n, here, :] = h
            pair[n, here, :] = two
            return result

        for zc in range(g.Z // 8):
            mean = [
                smooth(c, lambda d, c=c: pad[c, t + 2, 7 + 8 * zc + d : 15 + 8 * zc + d, :], zc)
                for c in range(3)
            ]
            field = lambda n: smooth(
                3 + n, lambda d: raw[slot, n, 8 * zc + d : 8 * zc + d + 8, :], zc
            )
            scaled = [m * 0.0625 for m in mean]
            leonard = [field(n) - scaled[a] * mean[b] for n, (a, b) in enumerate(PAIRS)]
            calm = [field(6 + n) for n in range(6)]
            size = size_of(calm) * (filter_ratio / 16.0)
            model = [size * calm[n] - field(12 + n) for n in range(6)]
            numer = leonard[0] * model[0]
            for n in range(1, 6):
                numer = numer + leonard[n] * model[n]
            diag = model[0] * model[0] + model[1] * model[1] + model[2] * model[2]
            side = model[3] * model[3] + model[4] * model[4] + model[5] * model[5]
            acc[0] += jnp.where(live, numer, 0.0)
            acc[1] += jnp.where(live, diag + 0.5 * side, 0.0)

    loop(g.T + 2, UNROLL_SUMS, step)
    w = width[...] * (2.0 / 16.0)
    numer = jnp.sum(acc[0], axis=0, keepdims=True) * (w[:1] * (1.0 / 16.0))
    denom = jnp.sum(acc[1], axis=0, keepdims=True) * (w[:1] * w[:1])
    index = lax.broadcasted_iota(jnp.int32, (8, g.R), 0)
    out[...] = jnp.where(index == 0, numer, jnp.where(index == 1, denom, 0.0))


def source_kernel(g, v, tlo, thi, zlo, zhi, width, sums, ratio, *rest):
    outs = rest[: g.chunks * g.ng]
    pad, tau, eddy, vt, vz, src, flip, sems, osems = rest[g.chunks * g.ng :]
    T, Z, R = g.T, g.Z, g.R
    fill_pad(g, v, tlo, thi, zlo, zhi, pad, sems)
    radius, inverse, up, down = g.lanes()
    rows = (inverse, up, down, g.kt * inverse)
    kt = rows[3]
    total = jnp.sum(sums[...], axis=0)
    coefficient = total[0:1] / (total[1:2] + epsilon_den)
    strength = jnp.broadcast_to(coefficient, (8, R)) * width[...]

    def stress_row(t, slot):
        for zc in range(eddy.shape[1] // 8):
            z = 6 + 8 * zc
            _, s = strain_rows(pad, t + 1, z, g, rows)
            e = strength * size_of(s)
            here = pl.ds(8 * zc, 8)
            eddy[t, here, :] = e * (1.0 / nu_molecular)
            side = time_step * (nu_molecular + e)
            main = side + side
            for n in range(3):
                tau[n, t, here, :] = main * s[n]
                tau[3 + n, t, here, :] = side * s[3 + n]

    loop(T + 4, UNROLL, stress_row)

    def slab(n, t, z):
        return tau[n, t, z : z + 8, :]

    def radial(f):
        return shift_up(f) * up - shift_down(f) * down

    def turn_row(a, slot):
        t = a + 1
        for zc in range(Z // 8):
            z = 2 + 8 * zc
            rt = slab(3, t, z)
            force = (
                radial(rt)
                + (slab(1, t + 1, z) - slab(1, t - 1, z)) * kt
                + (slab(5, t, z + 1) - slab(5, t, z - 1)) * g.kz
                + rt * (inverse + inverse)
            )
            vt[a, pl.ds(8 * zc, 8), :] = pad[1, a + 2, 8 + 8 * zc : 16 + 8 * zc, :] + force

    loop(T + 2, UNROLL, turn_row)
    r_up = shift_up(radius) * inverse * up
    r_down = shift_down(radius) * inverse * down

    def axial_row(a, slot):
        t = a + 2
        for zc in range(vz.shape[1] // 8):
            z = 1 + 8 * zc
            rz = slab(4, t, z)
            force = (
                radial(rz)
                + (slab(5, t + 1, z) - slab(5, t - 1, z)) * kt
                + (slab(2, t, z + 1) - slab(2, t, z - 1)) * g.kz
                + rz * inverse
            )
            vz[a, pl.ds(8 * zc, 8), :] = pad[2, a + 3, 7 + 8 * zc : 15 + 8 * zc, :] + force

    loop(T, UNROLL, axial_row)

    def radial_row(a, slot):
        t = a + 2
        for zc in range(Z // 8):
            z = 2 + 8 * zc
            rr = slab(0, t, z)
            force = (
                radial(rr)
                + (slab(3, t + 1, z) - slab(3, t - 1, z)) * kt
                + (slab(4, t, z + 1) - slab(4, t, z - 1)) * g.kz
                + (rr - slab(1, t, z)) * inverse
            )
            src[a, pl.ds(8 * zc, 8), :] = pad[0, a + 3, 8 + 8 * zc : 16 + 8 * zc, :] + force
            ratio[a, pl.ds(8 * zc, 8), :] = eddy[t, z : z + 8, :]

    loop(T, UNROLL, radial_row)

    def source_row(a, slot):
        for zc in range(Z // 8):
            here = pl.ds(8 * zc, 8)
            vr = src[a, here, :]
            src[a, here, :] = (
                shift_up(vr) * r_up
                - shift_down(vr) * r_down
                + (vt[a + 2, here, :] - vt[a, here, :]) * kt
                + (vz[a, 8 * zc + 2 : 8 * zc + 10, :] - vz[a, 8 * zc : 8 * zc + 8, :]) * g.kz
            )

    loop(T, UNROLL, source_row)
    flat = src.reshape(T * src.shape[1], R)
    turned = flip.reshape(R * flip.shape[1], 2 * T)

    def flip_step(p, slot):
        even = flat[pl.ds(2 * p, T, stride=src.shape[1]), :]
        odd = flat[pl.ds(2 * p + 1, T, stride=src.shape[1]), :]
        turned[pl.ds(p, R, stride=flip.shape[1]), :] = jnp.concatenate([even, odd], axis=0).T

    loop(Z // 2, UNROLL, flip_step)
    me = lax.axis_index("gz")
    copies = []
    for c in range(g.chunks):
        for s in range(g.ng):
            first = g.ng * g.first[c] + lax.rem(me + s, g.ng) * g.rb[c]
            n = c * g.ng + s
            copies.append(
                pltpu.make_async_copy(
                    flip.at[pl.ds(first, g.rb[c]), pl.ds(0, Z // 2), :], outs[n], osems.at[n]
                )
            )
    for copy in copies:
        copy.start()
    for copy in copies:
        copy.wait()


def split(x):
    parts = []
    for _ in range(2):
        parts.append(x.astype(jnp.bfloat16))
        x = x - parts[-1].astype(jnp.float32)
    return parts + [x.astype(jnp.bfloat16)]


def split_table(x):
    parts = []
    for _ in range(2):
        high = lax.reduce_precision(x, 8, 7)
        parts.append(high.astype(jnp.bfloat16))
        x = x - high
    return parts + [x.astype(jnp.bfloat16)]


def dot6(a, b):
    dot = functools.partial(jnp.dot, preferred_element_type=jnp.float32)
    small = dot(a[1], b[1]) + dot(a[2], b[0]) + dot(a[0], b[2])
    return dot(a[0], b[0]) + (dot(a[1], b[0]) + dot(a[0], b[1]) + small)


def axial_kernel(g, rb, *refs):
    blocks, tables = refs[: g.ng], refs[g.ng : g.ng + 3]
    outs = refs[g.ng + 3 : g.ng + 3 + g.nt]
    left = refs[g.ng + 3 + g.nt :]
    T, zp, kb = g.T, g.Z // 2, g.kb
    mine, other = lax.axis_index("gz"), lax.axis_index("theta")
    for s in range(g.ng):
        source = lax.rem(mine + g.ng - s, g.ng)
        for d in range(g.nt):
            target = lax.rem(other + d, g.nt)
            here = (pl.ds(d * kb, kb), pl.ds(4 * zp * s, 4 * zp))
            for n in range(3):
                left[n][here] = tables[n][source, target]
    per = 2 if rb % 2 == 0 else 1
    first = lax.broadcasted_iota(jnp.int32, (zp, 2 * T), 1) < T

    def column(r):
        parts = []
        for s in range(g.ng):
            x = blocks[s][r]
            y = jnp.concatenate([x[:, T:], x[:, :T]], axis=1)
            for f in (x, y):
                parts.append(jnp.where(first, f, 0.0))
                parts.append(jnp.where(first, 0.0, f))
        return jnp.concatenate(parts, axis=0)

    def step(i, carry):
        right = jnp.concatenate([column(per * i + q) for q in range(per)], axis=1)
        result = dot6([w[...] for w in left], split(right))
        for q in range(per):
            for d in range(g.nt):
                outs[d][per * i + q] = result[d * kb : (d + 1) * kb, q * 2 * T : (q + 1) * 2 * T]
        return carry

    lax.fori_loop(0, rb // per, step, 0)


def turn_kernel(g, rb, *refs):
    blocks, tables = refs[: g.nt], refs[g.nt : g.nt + 3]
    outs = refs[g.nt + 3 : g.nt + 3 + g.ng]
    mine, other = lax.axis_index("theta"), lax.axis_index("gz")
    rows = rb * g.kb
    left = split(jnp.concatenate([b[...].reshape(rows, 2 * g.T) for b in blocks], axis=1))
    for d in range(g.ng):
        target = lax.rem(other + d, g.ng)
        source = [lax.rem(mine + g.nt - s, g.nt) for s in range(g.nt)]
        right = [jnp.concatenate([w[target, s] for s in source], axis=0) for w in tables]
        result = dot6(left, right)
        for c in range(2):
            part = result[:, c * g.mb : (c + 1) * g.mb]
            outs[d][c] = part.reshape(rb, g.kb, g.mb)


def solve_kernel(g, *refs):
    count = g.chunks * g.ng
    blocks, coefs, out = refs[:count], refs[count], refs[count + 1]
    data, factor, flip, sems, osems = refs[count + 2 :]
    R, kb, mb = g.R, g.kb, g.mb
    mine, other = lax.axis_index("gz"), lax.axis_index("theta")
    copies = []
    for c in range(g.chunks):
        for s in range(g.ng):
            first = g.ng * g.first[c] + lax.rem(mine + g.ng - s, g.ng) * g.rb[c]
            n = c * g.ng + s
            copies.append(
                pltpu.make_async_copy(
                    blocks[n], data.at[:, pl.ds(first, g.rb[c]), pl.ds(0, kb), :], sems.at[n]
                )
            )
    for copy in copies:
        copy.start()
    for copy in copies:
        copy.wait()
    m = mine * mb + lax.broadcasted_iota(jnp.int32, (kb, mb), 1)
    k = other * kb + lax.broadcasted_iota(jnp.int32, (kb, mb), 0)
    a = jnp.minimum(m, g.NTH - m).astype(jnp.float32)
    q = jnp.minimum(k, g.NZ - k).astype(jnp.float32) * (2.0 * math.pi / pipe_length)
    a2, q2 = a * a, q * q
    zero = jnp.zeros((kb, mb), jnp.float32)

    def forward(r, carry):
        cp, re, im = carry
        lower, upper, centre, inv2 = (coefs[n, r] for n in range(4))
        w = 1.0 / ((centre - q2) - a2 * inv2 - lower * cp)
        cp = upper * w
        re = (data[0, r, :kb, :] - lower * re) * w
        im = (data[1, r, :kb, :] - lower * im) * w
        factor[r] = cp
        data[0, r, :kb, :] = re
        data[1, r, :kb, :] = im
        return cp, re, im

    lax.fori_loop(0, R, forward, (zero, zero, zero), unroll=4)

    def backward(i, carry):
        re, im = carry
        r = R - 1 - i
        cp = factor[r]
        re = data[0, r, :kb, :] - cp * re
        im = data[1, r, :kb, :] - cp * im
        data[0, r, :kb, :] = re
        data[1, r, :kb, :] = im
        return re, im

    lax.fori_loop(0, R, backward, (zero, zero), unroll=4)
    flat = data.reshape(2 * R * data.shape[2], mb)
    turned = flip.reshape(2 * mb * flip.shape[2], R)
    stores = []
    for c in range(2):

        def flip_step(i, slot, c=c):
            rows = flat[pl.ds(c * R * data.shape[2] + i, R, stride=data.shape[2]), :]
            turned[pl.ds(c * mb * flip.shape[2] + i, mb, stride=flip.shape[2]), :] = rows.T

        loop(kb, UNROLL, flip_step)
        copy = pltpu.make_async_copy(flip.at[c, :, pl.ds(0, kb), :], out.at[c], osems.at[c])
        copy.start()
        stores.append(copy)
    for copy in stores:
        copy.wait()


def exchange(blocks, axis):
    count = len(blocks)
    received = [blocks[0]]
    for s in range(1, count):
        ring = [(i, (i + s) % count) for i in range(count)]
        received.append(lax.ppermute(blocks[s], axis, ring))
    return received


def after(later, earlier):
    joined = lax.optimization_barrier((list(later), list(earlier)))
    return joined[0], joined[1]


def halo(g, v):
    T, Z = g.T, g.Z

    def pair(low, high, axis, count):
        forward = [(i, (i + 1) % count) for i in range(count)]
        backward = [(target, source) for source, target in forward]
        return lax.ppermute(high, axis, forward), lax.ppermute(low, axis, backward)

    tlo, thi = pair(v[:, :3], v[:, T - 3 :], "theta", g.nt)
    face = lambda first: jnp.concatenate(
        [f[:, :, first : first + 3].transpose(0, 2, 1, 3) for f in (tlo, v, thi)], axis=2
    )
    zlo, zhi = pair(face(0), face(Z - 3), "gz", g.ng)
    return tlo, thi, zlo, zhi


def axial_table(g):
    z, k = np.arange(g.NZ), np.arange(g.NZ)
    angle = 2.0 * math.pi * ((k[:, None] * z[None, :]) % g.NZ) / g.NZ
    scale = 1.0 / math.sqrt(g.NTH * g.NZ)
    cos = (np.cos(angle) * scale).reshape(g.nt, g.kb, g.ng, g.Z // 2, 2)
    sin = (-np.sin(angle) * scale).reshape(g.nt, g.kb, g.ng, g.Z // 2, 2)
    parts = [cos[..., 0], sin[..., 1], cos[..., 1], sin[..., 0]]
    table = np.stack(parts, axis=3).reshape(g.nt, g.kb, g.ng, 2 * g.Z)
    return split_table(jnp.asarray(table.transpose(2, 0, 1, 3).astype(np.float32)))


def turn_table(g):
    t, m = np.arange(g.T), np.arange(g.NTH)
    base = 2.0 * math.pi * ((t[:, None] * m[None, :]) % g.NTH) / g.NTH
    skip = 2.0 * math.pi * ((np.arange(g.nt)[:, None] * g.T * m[None, :]) % g.NTH) / g.NTH
    f32 = lambda x: jnp.asarray(x.astype(np.float32))
    fold = lambda x: x.reshape(x.shape[0], g.ng, g.mb).transpose(1, 0, 2)
    c0, s0 = f32(fold(np.cos(base)))[:, None], f32(fold(np.sin(base)))[:, None]
    c1, s1 = f32(fold(np.cos(skip)))[:, :, None], f32(fold(np.sin(skip)))[:, :, None]
    cos = c0 * c1 - s0 * s1
    sin = s0 * c1 + c0 * s1
    top = jnp.concatenate([cos, -sin], axis=-1)
    bottom = jnp.concatenate([sin, cos], axis=-1)
    return split_table(jnp.concatenate([top, bottom], axis=-2))


def solve_coefs(g):
    R = g.R
    radius = (np.arange(R) + 0.5) / R
    lower = (radius - 0.5 / R) / radius * (R * R)
    upper = (radius + 0.5 / R) / radius * (R * R)
    last = np.arange(R) == R - 1
    centre = -(lower + upper) - np.where(last, upper, 0.0)
    upper = np.where(last, 0.0, upper)
    return jnp.asarray(np.stack([lower, upper, centre, 1.0 / radius**2]).astype(np.float32))


def body(velocity):
    return program(Grid(velocity), velocity)


def program(g, velocity):
    T, Z, R, kb, mb = g.T, g.Z, g.R, g.kb, g.mb
    f32 = jnp.float32
    shape = lambda *s: jax.ShapeDtypeStruct(s, f32)
    buf = lambda *s: pltpu.VMEM(s, f32)
    dma = pltpu.SemaphoreType.DMA
    edges = halo(g, velocity)
    width = width_row(g)
    pad = buf(3, T + 6, odd_tiles(Z + 16), R)
    halo_specs = [ANY, ANY, ANY, VM, VM, VM]
    part = pl.pallas_call(
        functools.partial(sums_kernel, g),
        out_shape=shape(8, R),
        in_specs=halo_specs,
        out_specs=VM,
        scratch_shapes=[
            pad,
            buf(UNROLL_SUMS, 18, odd_tiles(Z + 2), R),
            buf(21, odd_tiles(Z), R),
            buf(21, odd_tiles(Z), R),
            buf(2, 8, R),
            dma((3,)),
        ],
        compiler_params=params(),
        name="germano_sums",
    )(velocity, *edges, width)
    count = g.nt * g.ng
    sums = lax.all_to_all(
        jnp.broadcast_to(part[None], (count, 8, R)), ("theta", "gz"), 0, 0, tiled=True
    )
    outs = pl.pallas_call(
        functools.partial(source_kernel, g),
        out_shape=[shape(T, Z, R)]
        + [shape(rb, Z // 2, 2 * T) for rb in g.rb for _ in range(g.ng)],
        in_specs=halo_specs + [VM],
        out_specs=[VM] + [ANY] * (g.chunks * g.ng),
        scratch_shapes=[
            pad,
            buf(6, T + 5, odd_tiles(Z + 10), R),
            buf(T + 4, round_up(Z + 4, 8), R),
            buf(T + 2, odd_tiles(Z), R),
            buf(T, round_up(Z + 2, 8), R),
            buf(T, Z + 8, R),
            buf(R, Z // 2 + 8, 2 * T),
            dma((3,)),
            dma((g.chunks * g.ng,)),
        ],
        compiler_params=params(),
        name="source",
    )(velocity, *edges, width, sums)
    ratio, pieces = outs[0], outs[1:]
    axial_tables = axial_table(g)
    turn_tables = turn_table(g)
    axials, modes = [], []
    for c, rb in enumerate(g.rb):
        piece = pieces[c * g.ng : (c + 1) * g.ng]
        if c >= 1:
            piece, axials[c - 1] = after(piece, axials[c - 1])
        line = exchange(piece, "gz")
        axial = pl.pallas_call(
            functools.partial(axial_kernel, g, rb),
            out_shape=[shape(rb, kb, 2 * T)] * g.nt,
            in_specs=[VM] * (g.ng + 3),
            out_specs=[VM] * g.nt,
            scratch_shapes=[pltpu.VMEM((g.NZ, 2 * g.NZ), jnp.bfloat16)] * 3,
            compiler_params=params(24 * 1024 * 1024),
            name="axial_modes",
        )(*line, *axial_tables)
        axials.append(axial)
    for c, rb in enumerate(g.rb):
        cycle = exchange(axials[c], "theta")
        turned = pl.pallas_call(
            functools.partial(turn_kernel, g, rb),
            out_shape=[shape(2, rb, kb, mb)] * g.ng,
            in_specs=[VM] * (g.nt + 3),
            out_specs=[VM] * g.ng,
            compiler_params=params(40 * 1024 * 1024),
            name="turn_modes",
        )(*cycle, *turn_tables)
        modes += exchange(turned, "gz")
    pressure = pl.pallas_call(
        functools.partial(solve_kernel, g),
        out_shape=shape(2, mb, kb, R),
        in_specs=[ANY] * len(modes) + [pl.BlockSpec(memory_space=pltpu.SMEM)],
        out_specs=ANY,
        scratch_shapes=[
            buf(2, R, kb + 8, mb),
            buf(R, kb, mb),
            buf(2, mb, kb + 8, R),
            dma((len(modes),)),
            dma((2,)),
        ],
        compiler_params=params(40 * 1024 * 1024),
        name="solve_modes",
    )(*modes, solve_coefs(g))
    return (ratio, pressure)


def solution(mesh):
    return jax.shard_map(
        body,
        mesh=mesh,
        in_specs=(P(None, "theta", "gz", None),),
        out_specs=(P("theta", "gz", None), P(None, "gz", "theta", None)),
        check_vma=False,
    )
```

```python
import functools
import math

import jax
import jax.numpy as jnp
import numpy as np
from jax import lax
from jax.experimental import pallas as pl
from jax.experimental.pallas import tpu as pltpu
from jax.sharding import PartitionSpec as P

pipe_length = 4.0 * math.pi
nu_molecular = 5e-05
time_step = 2.0
filter_ratio = 4.0
epsilon_den = 1e-06
CHUNK_EDGES = (0, 8, 16, 24, 32)
UNROLL = 4
SLOTS = 4
PARTS = 4
VMEM_BYTES = 60 * 1024 * 1024
ANY = pl.BlockSpec(memory_space=pl.ANY)
VM = pl.BlockSpec(memory_space=pltpu.VMEM)


def params(limit=VMEM_BYTES):
    return pltpu.CompilerParams(vmem_limit_bytes=limit)


def round_up(value, unit):
    return (value + unit - 1) // unit * unit


def odd_tiles(rows):
    return (round_up(rows, 8) // 8 | 1) * 8


def loop(count, most, step, before=None):
    unit = next(u for u in range(most, 0, -1) if count % u == 0)

    def several(i, carry):
        if before is not None:
            before(i, unit)
        for slot in range(unit):
            step(i * unit + slot, slot)
        return carry

    lax.fori_loop(0, count // unit, several, 0)


class Grid:
    def __init__(self, velocity):
        self.nt = lax.axis_size("theta")
        self.ng = lax.axis_size("gz")
        _, self.T, self.Z, self.R = velocity.shape
        self.chunks = len(CHUNK_EDGES) - 1
        self.NTH = self.T * self.nt
        self.NZ = self.Z * self.ng
        self.kb = self.NZ // self.nt
        self.mb = self.NTH // self.ng
        share = self.R // self.ng
        edges = [round(share * e / 32.0 / 2) * 2 for e in CHUNK_EDGES]
        self.first = edges[:-1]
        self.rb = [b - a for a, b in zip(edges, edges[1:])]
        self.kz = 0.5 * self.NZ / pipe_length
        self.kt = 0.5 * self.NTH / (2.0 * math.pi)

    def lanes(self):
        R = self.R
        index = lax.broadcasted_iota(jnp.int32, (8, R), 1)
        radius = (index.astype(jnp.float32) + 0.5) * (1.0 / R)
        inverse = 1.0 / radius
        up = jnp.where(index == R - 1, 0.0, 0.5 * R)
        down = jnp.where(index == 0, 0.0, 0.5 * R)
        return radius, inverse, up, down


def width_row(g):
    radius = (np.arange(g.R, dtype=np.float32) + np.float32(0.5)) * np.float32(1.0 / g.R)
    cell = radius.astype(np.float64) * (1.0 / g.R) * (2.0 * math.pi / g.NTH) * (pipe_length / g.NZ)
    return jnp.asarray(np.broadcast_to((np.cbrt(cell) ** 2).astype(np.float32), (8, g.R)))


def shift_up(f):
    return pltpu.roll(f, f.shape[-1] - 1, 1)


def shift_down(f):
    return pltpu.roll(f, 1, 1)


def strain_rows(fetch, t, z, g, rows):
    inverse, up, down, kt = rows
    at = lambda c, dt, dz: fetch(c, t + dt, z + dz)
    u = [at(c, 0, 0) for c in range(3)]
    radial = [shift_up(f) * up - shift_down(f) * down for f in u]
    turn = [(at(c, 1, 0) - at(c, -1, 0)) * kt for c in range(3)]
    axial = [(at(c, 0, 1) - at(c, 0, -1)) * g.kz for c in range(3)]
    ur, ut = u[0] * inverse, u[1] * inverse
    s = [
        radial[0],
        turn[1] + ur,
        axial[2],
        radial[1] - ut + turn[0],
        axial[0] + radial[2],
        turn[2] + axial[1],
    ]
    return u, s


def root(x):
    return x * lax.rsqrt(jnp.maximum(x, 1e-36))


def size_of(s):
    diag = s[0] * s[0] + s[1] * s[1] + s[2] * s[2]
    return root((diag + diag) + (s[3] * s[3] + s[4] * s[4] + s[5] * s[5]))


def put_columns(pad, block, row, z, values):
    *_, height, pitch, R = pad.shape
    flat = pad.reshape(math.prod(pad.shape[:-1]), R)
    which = block[0] if len(block) == 1 else block[0] * 3 + block[1]
    flat[pl.ds((which * height + row) * pitch + z, values.shape[0], stride=pitch), :] = values


def fill_pad(g, v, edges, pad, sems):
    T, Z = g.T, g.Z
    tlo, thi, zlo, zhi, *corners = edges
    block = row_copies(v, pad, 3, sems)
    copies = [
        pltpu.make_async_copy(tlo, pad.at[:, pl.ds(0, 3), pl.ds(8, Z), :], sems.at[PARTS]),
        pltpu.make_async_copy(thi, pad.at[:, pl.ds(T + 3, 3), pl.ds(8, Z), :], sems.at[PARTS + 1]),
    ]
    for copy in copies + block:
        copy.start()
    for c in range(3):
        for i in range(3):
            for z, face, low, high in (
                (5 + i, zlo, corners[0], corners[2]),
                (8 + Z + i, zhi, corners[1], corners[3]),
            ):
                put_columns(pad, (c,), 0, z, low[c, i])
                put_columns(pad, (c,), 3, z, face[c, i])
                put_columns(pad, (c,), T + 3, z, high[c, i])
    for copy in copies:
        copy.wait()
    return block


PAIRS = ((0, 0), (1, 1), (2, 2), (0, 1), (0, 2), (1, 2))


def germano_pass(g, fetch, first, count, raws, filters, refs, unit=1, before=None):
    raw, last, pair, acc = refs
    _, inverse, up, down = g.lanes()
    rows = (inverse, up, down, g.kt * inverse)
    index = lax.broadcasted_iota(jnp.int32, (8, g.R), 0)

    def products(t, slot):
        for z, place in raws:
            u, s = strain_rows(fetch, t, z, g, rows)
            size = size_of(s)
            here = pl.ds(place, 8)
            for n, (a, b) in enumerate(PAIRS):
                raw[slot, n, here, :] = u[a] * u[b]
                raw[slot, 6 + n, here, :] = s[n]
                raw[slot, 12 + n, here, :] = size * s[n]

    def smooth(n, load, m):
        centre = load(1)
        h = (load(0) + load(2)) + (centre + centre)
        here = pl.ds(8 * m, 8)
        two = last[n, here, :] + h
        result = pair[n, here, :] + two
        last[n, here, :] = h
        pair[n, here, :] = two
        return result

    def contract(i, t, slot):
        for m, (z, place, keep) in enumerate(filters):
            mean = [smooth(c, lambda d, c=c: fetch(c, t, z - 1 + d), m) for c in range(3)]
            field = lambda n: smooth(
                3 + n, lambda d: raw[slot, n, place + d : place + d + 8, :], m
            )
            scaled = [f * 0.0625 for f in mean]
            leonard = [field(n) - scaled[a] * mean[b] for n, (a, b) in enumerate(PAIRS)]
            calm = [field(6 + n) for n in range(6)]
            size = size_of(calm) * (filter_ratio / 16.0)
            model = [size * calm[n] - field(12 + n) for n in range(6)]
            numer = leonard[0] * model[0]
            for n in range(1, 6):
                numer = numer + leonard[n] * model[n]
            diag = model[0] * model[0] + model[1] * model[1] + model[2] * model[2]
            side = model[3] * model[3] + model[4] * model[4] + model[5] * model[5]
            live = index < jnp.where((i >= 2) & (i < count + 2), keep, 0)
            acc[0] += jnp.where(live, numer, 0.0)
            acc[1] += jnp.where(live, diag + 0.5 * side, 0.0)

    def step(i, carry):
        if before is not None:
            before(i)
        for slot in range(unit):
            products(first - 1 + i * unit + slot, slot)
        for slot in range(unit):
            contract(i * unit + slot, first - 1 + i * unit + slot, slot)
        return carry

    lax.fori_loop(0, (count + 1 + unit) // unit, step, 0)


def row_copies(source, target, first, sems):
    part = source.shape[1] // PARTS
    return [
        pltpu.make_async_copy(
            source.at[:, pl.ds(p * part, part), :, :],
            target.at[:, pl.ds(first + p * part, part), pl.ds(0 if first == 0 else 8, source.shape[2]), :],
            sems.at[p],
        )
        for p in range(PARTS)
    ]


def inner_kernel(g, source, out, v, raw, last, pair, sems):
    copies = row_copies(source, v, 0, sems)
    for copy in copies:
        copy.start()
    out[...] = jnp.zeros_like(out)
    starts = list(range(3, g.Z - 9, 8)) + [g.Z - 9]
    part = g.T // PARTS
    copies[0].wait()

    def before(i):
        for p in range(1, PARTS):
            pl.when(i == p * part - 2)(copies[p].wait)

    germano_pass(
        g,
        lambda c, t, z: v[c, t, z : z + 8, :],
        2,
        g.T - 4,
        [(z, z - 3) for z in starts],
        [(4 + 8 * m, 8 * m, 8) for m in range(g.Z // 8 - 1)],
        (raw, last, pair, out),
        before=before,
    )


def edge_kernel(g, v, *refs):
    edges, (inner, width, out) = refs[:8], refs[8:11]
    ends, strip, raw, last, pair, acc, sems = refs[11:]
    low, high = ends.at[0], ends.at[1]
    T, Z = g.T, g.Z
    tlo, thi, zlo, zhi, *corners = edges
    wide = pl.ds(8, Z)
    pieces = (
        (v.at[:, :, pl.ds(0, 8), :], strip.at[:, pl.ds(0, T), pl.ds(8, 8), :]),
        (v.at[:, :, pl.ds(Z - 8, 8), :], strip.at[:, pl.ds(0, T), pl.ds(16, 8), :]),
        (tlo, low.at[:, pl.ds(0, 3), wide, :]),
        (v.at[:, pl.ds(0, 4), :, :], low.at[:, pl.ds(3, 4), wide, :]),
        (v.at[:, pl.ds(T - 4, 4), :, :], high.at[:, pl.ds(1, 4), wide, :]),
        (thi, high.at[:, pl.ds(5, 3), wide, :]),
    )
    copies = [pltpu.make_async_copy(a, b, sems.at[n]) for n, (a, b) in enumerate(pieces)]
    for copy in copies:
        copy.start()
    for c in range(3):
        for i in range(3):
            for n, face in enumerate((zlo, zhi)):
                put_columns(strip, (c,), 0, (5, 24)[n] + i, face[c, i])
                z = (5, 8 + Z)[n] + i
                put_columns(ends, (0, c), 0, z, corners[n][c, i])
                put_columns(ends, (0, c), 3, z, face[c, i, :4])
                put_columns(ends, (1, c), 1, z, face[c, i, T - 4 :])
                put_columns(ends, (1, c), 5, z, corners[2 + n][c, i])
    acc[...] = inner[...]
    for copy in copies:
        copy.wait()
    work = (raw, last, pair, acc)

    def near(c, t, z):
        place = z + 8 if z < Z // 2 else z - Z + 24
        return strip[c, t, place : place + 8, :]

    germano_pass(
        g,
        near,
        2,
        T - 4,
        [(-1, 0), (Z - 5, 16)],
        [(0, 0, 4), (Z - 4, 16, 4)],
        work,
        unit=SLOTS,
    )
    raws = [(8 * k - 1, 8 * k) for k in range(Z // 8 + 1)]
    filters = [(8 * m, 8 * m, 8) for m in range(Z // 8)]

    def end(which, carry):
        fetch = lambda c, t, z: ends[which, c, t + 3, z + 8 : z + 16, :]
        germano_pass(g, fetch, 0, 2, raws, filters, work)
        return carry

    lax.fori_loop(0, 2, end, 0)
    w = width[...] * (2.0 / 16.0)
    numer = jnp.sum(acc[0], axis=0, keepdims=True) * (w[:1] * (1.0 / 16.0))
    denom = jnp.sum(acc[1], axis=0, keepdims=True) * (w[:1] * w[:1])
    index = lax.broadcasted_iota(jnp.int32, (8, g.R), 0)
    out[...] = jnp.where(index == 0, numer, jnp.where(index == 1, denom, 0.0))


def source_kernel(g, v, *refs):
    edges, (width, sums, ratio), rest = refs[:8], refs[8:11], refs[11:]
    outs = rest[: g.chunks * g.ng]
    pad, tau, eddy, vt, vz, src, flip, sems, osems = rest[g.chunks * g.ng :]
    T, Z, R = g.T, g.Z, g.R
    block = fill_pad(g, v, edges, pad, sems)
    block[0].wait()
    radius, inverse, up, down = g.lanes()
    rows = (inverse, up, down, g.kt * inverse)
    kt = rows[3]
    total = jnp.sum(sums[...], axis=0)
    coefficient = total[0:1] / (total[1:2] + epsilon_den)
    strength = jnp.broadcast_to(coefficient, (8, R)) * width[...]

    fetch = lambda c, t, z: pad[c, t + 3, z + 8 : z + 16, :]

    def stress_row(t, slot):
        for zc in range(eddy.shape[1] // 8):
            _, s = strain_rows(fetch, t - 2, 8 * zc - 2, g, rows)
            e = strength * size_of(s)
            here = pl.ds(8 * zc, 8)
            eddy[t, here, :] = e * (1.0 / nu_molecular)
            side = time_step * (nu_molecular + e)
            main = side + side
            for n in range(3):
                tau[n, t, here, :] = main * s[n]
                tau[3 + n, t, here, :] = side * s[3 + n]

    def arrived(i, unit):
        for p in range(1, PARTS):
            pl.when(i == -(-(p * (T // PARTS) + 2 - unit) // unit))(block[p].wait)

    loop(T + 4, UNROLL, stress_row, arrived)

    def slab(n, t, z):
        return tau[n, t, z : z + 8, :]

    def radial(f):
        return shift_up(f) * up - shift_down(f) * down

    def turn_row(a, slot):
        t = a + 1
        for zc in range(Z // 8):
            z = 2 + 8 * zc
            rt = slab(3, t, z)
            force = (
                radial(rt)
                + (slab(1, t + 1, z) - slab(1, t - 1, z)) * kt
                + (slab(5, t, z + 1) - slab(5, t, z - 1)) * g.kz
                + rt * (inverse + inverse)
            )
            vt[a, pl.ds(8 * zc, 8), :] = pad[1, a + 2, 8 + 8 * zc : 16 + 8 * zc, :] + force

    loop(T + 2, UNROLL, turn_row)
    r_up = shift_up(radius) * inverse * up
    r_down = shift_down(radius) * inverse * down

    def axial_row(a, slot):
        t = a + 2
        for zc in range(vz.shape[1] // 8):
            z = 1 + 8 * zc
            rz = slab(4, t, z)
            force = (
                radial(rz)
                + (slab(5, t + 1, z) - slab(5, t - 1, z)) * kt
                + (slab(2, t, z + 1) - slab(2, t, z - 1)) * g.kz
                + rz * inverse
            )
            vz[a, pl.ds(8 * zc, 8), :] = pad[2, a + 3, 7 + 8 * zc : 15 + 8 * zc, :] + force

    loop(T, UNROLL, axial_row)

    def radial_row(a, slot):
        t = a + 2
        for zc in range(Z // 8):
            z = 2 + 8 * zc
            rr = slab(0, t, z)
            force = (
                radial(rr)
                + (slab(3, t + 1, z) - slab(3, t - 1, z)) * kt
                + (slab(4, t, z + 1) - slab(4, t, z - 1)) * g.kz
                + (rr - slab(1, t, z)) * inverse
            )
            src[a, pl.ds(8 * zc, 8), :] = pad[0, a + 3, 8 + 8 * zc : 16 + 8 * zc, :] + force
            ratio[a, pl.ds(8 * zc, 8), :] = eddy[t, z : z + 8, :]

    loop(T, UNROLL, radial_row)

    def source_row(a, slot):
        for zc in range(Z // 8):
            here = pl.ds(8 * zc, 8)
            vr = src[a, here, :]
            src[a, here, :] = (
                shift_up(vr) * r_up
                - shift_down(vr) * r_down
                + (vt[a + 2, here, :] - vt[a, here, :]) * kt
                + (vz[a, 8 * zc + 2 : 8 * zc + 10, :] - vz[a, 8 * zc : 8 * zc + 8, :]) * g.kz
            )

    loop(T, UNROLL, source_row)
    flat = src.reshape(T * src.shape[1], R)
    turned = flip.reshape(R * flip.shape[1], 2 * T)

    def flip_step(p, slot):
        even = flat[pl.ds(2 * p, T, stride=src.shape[1]), :]
        odd = flat[pl.ds(2 * p + 1, T, stride=src.shape[1]), :]
        turned[pl.ds(p, R, stride=flip.shape[1]), :] = jnp.concatenate([even, odd], axis=0).T

    loop(Z // 2, UNROLL, flip_step)
    me = lax.axis_index("gz")
    copies = []
    for c in range(g.chunks):
        for s in range(g.ng):
            first = g.ng * g.first[c] + lax.rem(me + s, g.ng) * g.rb[c]
            n = c * g.ng + s
            copies.append(
                pltpu.make_async_copy(
                    flip.at[pl.ds(first, g.rb[c]), pl.ds(0, Z // 2), :], outs[n], osems.at[n]
                )
            )
    for copy in copies:
        copy.start()
    for copy in copies:
        copy.wait()


def split(x):
    parts = []
    for _ in range(2):
        parts.append(x.astype(jnp.bfloat16))
        x = x - parts[-1].astype(jnp.float32)
    return parts + [x.astype(jnp.bfloat16)]


def split_table(x):
    parts = []
    for _ in range(2):
        high = lax.reduce_precision(x, 8, 7)
        parts.append(high.astype(jnp.bfloat16))
        x = x - high
    return parts + [x.astype(jnp.bfloat16)]


def dot6(a, b):
    dot = functools.partial(jnp.dot, preferred_element_type=jnp.float32)
    small = dot(a[1], b[1]) + dot(a[2], b[0]) + dot(a[0], b[2])
    return dot(a[0], b[0]) + (dot(a[1], b[0]) + dot(a[0], b[1]) + small)


def axial_kernel(g, rb, *refs):
    blocks, tables = refs[: g.ng], refs[g.ng : g.ng + 3]
    outs = refs[g.ng + 3 : g.ng + 3 + g.nt]
    left = refs[g.ng + 3 + g.nt :]
    T, zp, kb = g.T, g.Z // 2, g.kb
    mine, other = lax.axis_index("gz"), lax.axis_index("theta")
    for s in range(g.ng):
        source = lax.rem(mine + g.ng - s, g.ng)
        for d in range(g.nt):
            target = lax.rem(other + d, g.nt)
            here = (pl.ds(d * kb, kb), pl.ds(4 * zp * s, 4 * zp))
            for n in range(3):
                left[n][here] = tables[n][source, target]
    per = 2 if rb % 2 == 0 else 1
    first = lax.broadcasted_iota(jnp.int32, (zp, 2 * T), 1) < T

    def column(r):
        parts = []
        for s in range(g.ng):
            x = blocks[s][r]
            y = jnp.concatenate([x[:, T:], x[:, :T]], axis=1)
            for f in (x, y):
                parts.append(jnp.where(first, f, 0.0))
                parts.append(jnp.where(first, 0.0, f))
        return jnp.concatenate(parts, axis=0)

    def step(i, carry):
        right = jnp.concatenate([column(per * i + q) for q in range(per)], axis=1)
        result = dot6([w[...] for w in left], split(right))
        for q in range(per):
            for d in range(g.nt):
                outs[d][per * i + q] = result[d * kb : (d + 1) * kb, q * 2 * T : (q + 1) * 2 * T]
        return carry

    lax.fori_loop(0, rb // per, step, 0)


def turn_kernel(g, rb, *refs):
    blocks, tables = refs[: g.nt], refs[g.nt : g.nt + 3]
    outs = refs[g.nt + 3 : g.nt + 3 + g.ng]
    mine, other = lax.axis_index("theta"), lax.axis_index("gz")
    rows = rb * g.kb
    left = split(jnp.concatenate([b[...].reshape(rows, 2 * g.T) for b in blocks], axis=1))
    for d in range(g.ng):
        target = lax.rem(other + d, g.ng)
        source = [lax.rem(mine + g.nt - s, g.nt) for s in range(g.nt)]
        right = [jnp.concatenate([w[target, s] for s in source], axis=0) for w in tables]
        result = dot6(left, right)
        for c in range(2):
            part = result[:, c * g.mb : (c + 1) * g.mb]
            outs[d][c] = part.reshape(rb, g.kb, g.mb)


def solve_kernel(g, *refs):
    count = g.chunks * g.ng
    blocks, coefs, out = refs[:count], refs[count], refs[count + 1]
    data, factor, flip, sems, osems = refs[count + 2 :]
    R, kb, mb = g.R, g.kb, g.mb
    mine, other = lax.axis_index("gz"), lax.axis_index("theta")
    copies = []
    for c in range(g.chunks):
        for s in range(g.ng):
            first = g.ng * g.first[c] + lax.rem(mine + g.ng - s, g.ng) * g.rb[c]
            n = c * g.ng + s
            copies.append(
                pltpu.make_async_copy(
                    blocks[n], data.at[:, pl.ds(first, g.rb[c]), pl.ds(0, kb), :], sems.at[n]
                )
            )
    for copy in copies:
        copy.start()
    for copy in copies:
        copy.wait()
    m = mine * mb + lax.broadcasted_iota(jnp.int32, (kb, mb), 1)
    k = other * kb + lax.broadcasted_iota(jnp.int32, (kb, mb), 0)
    a = jnp.minimum(m, g.NTH - m).astype(jnp.float32)
    q = jnp.minimum(k, g.NZ - k).astype(jnp.float32) * (2.0 * math.pi / pipe_length)
    a2, q2 = a * a, q * q
    zero = jnp.zeros((kb, mb), jnp.float32)

    def forward(r, carry):
        cp, re, im = carry
        lower, upper, centre, inv2 = (coefs[n, r] for n in range(4))
        w = 1.0 / ((centre - q2) - a2 * inv2 - lower * cp)
        cp = upper * w
        re = (data[0, r, :kb, :] - lower * re) * w
        im = (data[1, r, :kb, :] - lower * im) * w
        factor[r] = cp
        data[0, r, :kb, :] = re
        data[1, r, :kb, :] = im
        return cp, re, im

    lax.fori_loop(0, R, forward, (zero, zero, zero), unroll=4)

    def backward(i, carry):
        re, im = carry
        r = R - 1 - i
        cp = factor[r]
        re = data[0, r, :kb, :] - cp * re
        im = data[1, r, :kb, :] - cp * im
        data[0, r, :kb, :] = re
        data[1, r, :kb, :] = im
        return re, im

    lax.fori_loop(0, R, backward, (zero, zero), unroll=4)
    flat = data.reshape(2 * R * data.shape[2], mb)
    turned = flip.reshape(2 * mb * flip.shape[2], R)
    stores = []
    for c in range(2):

        def flip_step(i, slot, c=c):
            rows = flat[pl.ds(c * R * data.shape[2] + i, R, stride=data.shape[2]), :]
            turned[pl.ds(c * mb * flip.shape[2] + i, mb, stride=flip.shape[2]), :] = rows.T

        loop(kb, UNROLL, flip_step)
        copy = pltpu.make_async_copy(flip.at[c, :, pl.ds(0, kb), :], out.at[c], osems.at[c])
        copy.start()
        stores.append(copy)
    for copy in stores:
        copy.wait()


def exchange(blocks, axis):
    count = len(blocks)
    received = [blocks[0]]
    for s in range(1, count):
        ring = [(i, (i + s) % count) for i in range(count)]
        received.append(lax.ppermute(blocks[s], axis, ring))
    return received


def after(later, earlier):
    joined = lax.optimization_barrier((list(later), list(earlier)))
    return joined[0], joined[1]


def halo(g, v):
    T, Z = g.T, g.Z

    def move(block, dt, dz):
        ring = [
            (t * g.ng + z, (t + dt) % g.nt * g.ng + (z + dz) % g.ng)
            for t in range(g.nt)
            for z in range(g.ng)
        ]
        return lax.ppermute(block, ("theta", "gz"), ring)

    first = v[:, :, :3].transpose(0, 2, 1, 3)
    final = v[:, :, Z - 3 :].transpose(0, 2, 1, 3)
    faces = [
        move(final, 0, 1), move(first, 0, -1), move(v[:, T - 3 :], 1, 0), move(v[:, :3], -1, 0)
    ]
    corners = [
        move(final[:, :, T - 3 :], 1, 1),
        move(first[:, :, T - 3 :], 1, -1),
        move(final[:, :, :3], -1, 1),
        move(first[:, :, :3], -1, -1),
    ]
    return faces[2], faces[3], faces[0], faces[1], *corners


def axial_table(g):
    z, k = np.arange(g.NZ), np.arange(g.NZ)
    angle = 2.0 * math.pi * ((k[:, None] * z[None, :]) % g.NZ) / g.NZ
    scale = 1.0 / math.sqrt(g.NTH * g.NZ)
    cos = (np.cos(angle) * scale).reshape(g.nt, g.kb, g.ng, g.Z // 2, 2)
    sin = (-np.sin(angle) * scale).reshape(g.nt, g.kb, g.ng, g.Z // 2, 2)
    parts = [cos[..., 0], sin[..., 1], cos[..., 1], sin[..., 0]]
    table = np.stack(parts, axis=3).reshape(g.nt, g.kb, g.ng, 2 * g.Z)
    return split_table(jnp.asarray(table.transpose(2, 0, 1, 3).astype(np.float32)))


def turn_table(g):
    t, m = np.arange(g.T), np.arange(g.NTH)
    base = 2.0 * math.pi * ((t[:, None] * m[None, :]) % g.NTH) / g.NTH
    skip = 2.0 * math.pi * ((np.arange(g.nt)[:, None] * g.T * m[None, :]) % g.NTH) / g.NTH
    f32 = lambda x: jnp.asarray(x.astype(np.float32))
    fold = lambda x: x.reshape(x.shape[0], g.ng, g.mb).transpose(1, 0, 2)
    c0, s0 = f32(fold(np.cos(base)))[:, None], f32(fold(np.sin(base)))[:, None]
    c1, s1 = f32(fold(np.cos(skip)))[:, :, None], f32(fold(np.sin(skip)))[:, :, None]
    cos = c0 * c1 - s0 * s1
    sin = s0 * c1 + c0 * s1
    top = jnp.concatenate([cos, -sin], axis=-1)
    bottom = jnp.concatenate([sin, cos], axis=-1)
    return split_table(jnp.concatenate([top, bottom], axis=-2))


def solve_coefs(g):
    R = g.R
    radius = (np.arange(R) + 0.5) / R
    lower = (radius - 0.5 / R) / radius * (R * R)
    upper = (radius + 0.5 / R) / radius * (R * R)
    last = np.arange(R) == R - 1
    centre = -(lower + upper) - np.where(last, upper, 0.0)
    upper = np.where(last, 0.0, upper)
    return jnp.asarray(np.stack([lower, upper, centre, 1.0 / radius**2]).astype(np.float32))


def body(velocity):
    return program(Grid(velocity), velocity)


def program(g, velocity):
    T, Z, R, kb, mb = g.T, g.Z, g.R, g.kb, g.mb
    f32 = jnp.float32
    shape = lambda *s: jax.ShapeDtypeStruct(s, f32)
    buf = lambda *s: pltpu.VMEM(s, f32)
    dma = pltpu.SemaphoreType.DMA
    edges = halo(g, velocity)
    width = width_row(g)
    pad = buf(3, T + 6, odd_tiles(Z + 16), R)
    halo_specs = [ANY, ANY, ANY] + [VM] * 6
    work = [buf(SLOTS, 18, odd_tiles(Z + 2), R), buf(21, odd_tiles(Z), R), buf(21, odd_tiles(Z), R)]
    inner = pl.pallas_call(
        functools.partial(inner_kernel, g),
        out_shape=shape(2, 8, R),
        in_specs=[ANY],
        out_specs=VM,
        scratch_shapes=[buf(3, T, Z, R), *work, dma((PARTS,))],
        compiler_params=params(50 * 1024 * 1024),
        name="inner_sums",
    )(velocity)
    part = pl.pallas_call(
        functools.partial(edge_kernel, g),
        out_shape=shape(8, R),
        in_specs=[ANY, ANY, ANY] + [VM] * 8,
        out_specs=VM,
        scratch_shapes=[
            buf(2, 3, 8, odd_tiles(Z + 16), R),
            buf(3, T + 2, 40, R),
            *work,
            buf(2, 8, R),
            dma((6,)),
        ],
        compiler_params=params(40 * 1024 * 1024),
        name="edge_sums",
    )(velocity, *edges, inner, width)
    count = g.nt * g.ng
    sums = lax.all_to_all(
        jnp.broadcast_to(part[None], (count, 8, R)), ("theta", "gz"), 0, 0, tiled=True
    )
    outs = pl.pallas_call(
        functools.partial(source_kernel, g),
        out_shape=[shape(T, Z, R)]
        + [shape(rb, Z // 2, 2 * T) for rb in g.rb for _ in range(g.ng)],
        in_specs=halo_specs + [VM] * 2,
        out_specs=[VM] + [ANY] * (g.chunks * g.ng),
        scratch_shapes=[
            pad,
            buf(6, T + 5, odd_tiles(Z + 10), R),
            buf(T + 4, round_up(Z + 4, 8), R),
            buf(T + 2, odd_tiles(Z), R),
            buf(T, round_up(Z + 2, 8), R),
            buf(T, Z + 8, R),
            buf(R, Z // 2 + 8, 2 * T),
            dma((PARTS + 2,)),
            dma((g.chunks * g.ng,)),
        ],
        compiler_params=params(),
        name="source",
    )(velocity, *edges, width, sums)
    ratio, pieces = outs[0], outs[1:]
    axial_tables = axial_table(g)
    turn_tables = turn_table(g)
    axials, modes = [], []
    for c, rb in enumerate(g.rb):
        piece = pieces[c * g.ng : (c + 1) * g.ng]
        if c >= 1:
            piece, axials[c - 1] = after(piece, axials[c - 1])
        line = exchange(piece, "gz")
        axial = pl.pallas_call(
            functools.partial(axial_kernel, g, rb),
            out_shape=[shape(rb, kb, 2 * T)] * g.nt,
            in_specs=[VM] * (g.ng + 3),
            out_specs=[VM] * g.nt,
            scratch_shapes=[pltpu.VMEM((g.NZ, 2 * g.NZ), jnp.bfloat16)] * 3,
            compiler_params=params(24 * 1024 * 1024),
            name="axial_modes",
        )(*line, *axial_tables)
        axials.append(axial)
    for c, rb in enumerate(g.rb):
        cycle = exchange(axials[c], "theta")
        turned = pl.pallas_call(
            functools.partial(turn_kernel, g, rb),
            out_shape=[shape(2, rb, kb, mb)] * g.ng,
            in_specs=[VM] * (g.nt + 3),
            out_specs=[VM] * g.ng,
            compiler_params=params(40 * 1024 * 1024),
            name="turn_modes",
        )(*cycle, *turn_tables)
        modes += exchange(turned, "gz")
    pressure = pl.pallas_call(
        functools.partial(solve_kernel, g),
        out_shape=shape(2, mb, kb, R),
        in_specs=[ANY] * len(modes) + [pl.BlockSpec(memory_space=pltpu.SMEM)],
        out_specs=ANY,
        scratch_shapes=[
            buf(2, R, kb + 8, mb),
            buf(R, kb, mb),
            buf(2, mb, kb + 8, R),
            dma((len(modes),)),
            dma((2,)),
        ],
        compiler_params=params(40 * 1024 * 1024),
        name="solve_modes",
    )(*modes, solve_coefs(g))
    return (ratio, pressure)


def solution(mesh):
    return jax.shard_map(
        body,
        mesh=mesh,
        in_specs=(P(None, "theta", "gz", None),),
        out_specs=(P("theta", "gz", None), P(None, "gz", "theta", None)),
        check_vma=False,
    )
```

```python
import functools
import math

import jax
import jax.numpy as jnp
import numpy as np
from jax import lax
from jax.experimental import pallas as pl
from jax.experimental.pallas import tpu as pltpu
from jax.sharding import PartitionSpec as P

pipe_length = 4.0 * math.pi
nu_molecular = 5e-05
time_step = 2.0
filter_ratio = 4.0
epsilon_den = 1e-06
CHUNK_EDGES = (0, 8, 18, 26, 32)
UNROLL = 4
SLOTS = 4
PARTS = 4
VMEM_BYTES = 60 * 1024 * 1024
ANY = pl.BlockSpec(memory_space=pl.ANY)
VM = pl.BlockSpec(memory_space=pltpu.VMEM)


def params(limit=VMEM_BYTES):
    return pltpu.CompilerParams(vmem_limit_bytes=limit)


def round_up(value, unit):
    return (value + unit - 1) // unit * unit


def odd_tiles(rows):
    return (round_up(rows, 8) // 8 | 1) * 8


def loop(count, most, step, before=None):
    unit = next(u for u in range(most, 0, -1) if count % u == 0)

    def several(i, carry):
        if before is not None:
            before(i, unit)
        for slot in range(unit):
            step(i * unit + slot, slot)
        return carry

    lax.fori_loop(0, count // unit, several, 0)


class Grid:
    def __init__(self, velocity):
        self.nt = lax.axis_size("theta")
        self.ng = lax.axis_size("gz")
        _, self.T, self.Z, self.R = velocity.shape
        self.chunks = len(CHUNK_EDGES) - 1
        self.NTH = self.T * self.nt
        self.NZ = self.Z * self.ng
        self.kb = self.NZ // self.nt
        self.mb = self.NTH // self.ng
        share = self.R // self.ng
        edges = [round(share * e / 32.0 / 2) * 2 for e in CHUNK_EDGES]
        self.first = edges[:-1]
        self.rb = [b - a for a, b in zip(edges, edges[1:])]
        self.kz = 0.5 * self.NZ / pipe_length
        self.kt = 0.5 * self.NTH / (2.0 * math.pi)

    def lanes(self):
        R = self.R
        index = lax.broadcasted_iota(jnp.int32, (8, R), 1)
        radius = (index.astype(jnp.float32) + 0.5) * (1.0 / R)
        inverse = 1.0 / radius
        up = jnp.where(index == R - 1, 0.0, 0.5 * R)
        down = jnp.where(index == 0, 0.0, 0.5 * R)
        return radius, inverse, up, down


def width_row(g):
    radius = (np.arange(g.R, dtype=np.float32) + np.float32(0.5)) * np.float32(1.0 / g.R)
    cell = radius.astype(np.float64) * (1.0 / g.R) * (2.0 * math.pi / g.NTH) * (pipe_length / g.NZ)
    return jnp.asarray(np.broadcast_to((np.cbrt(cell) ** 2).astype(np.float32), (8, g.R)))


def shift_up(f):
    return pltpu.roll(f, f.shape[-1] - 1, 1)


def shift_down(f):
    return pltpu.roll(f, 1, 1)


def strain_rows(fetch, t, z, g, rows):
    inverse, up, down, kt = rows
    at = lambda c, dt, dz: fetch(c, t + dt, z + dz)
    u = [at(c, 0, 0) for c in range(3)]
    radial = [shift_up(f) * up - shift_down(f) * down for f in u]
    turn = [(at(c, 1, 0) - at(c, -1, 0)) * kt for c in range(3)]
    axial = [(at(c, 0, 1) - at(c, 0, -1)) * g.kz for c in range(3)]
    ur, ut = u[0] * inverse, u[1] * inverse
    s = [
        radial[0],
        turn[1] + ur,
        axial[2],
        radial[1] - ut + turn[0],
        axial[0] + radial[2],
        turn[2] + axial[1],
    ]
    return u, s


def root(x):
    return x * lax.rsqrt(jnp.maximum(x, 1e-36))


def size_of(s):
    diag = s[0] * s[0] + s[1] * s[1] + s[2] * s[2]
    return root((diag + diag) + (s[3] * s[3] + s[4] * s[4] + s[5] * s[5]))


def put_columns(pad, block, row, z, values):
    *_, height, pitch, R = pad.shape
    flat = pad.reshape(math.prod(pad.shape[:-1]), R)
    which = block[0] if len(block) == 1 else block[0] * 3 + block[1]
    flat[pl.ds((which * height + row) * pitch + z, values.shape[0], stride=pitch), :] = values


def fill_pad(g, v, edges, pad, sems):
    T, Z = g.T, g.Z
    tlo, thi, zlo, zhi, *corners = edges
    block = row_copies(v, pad, 3, sems)
    copies = [
        pltpu.make_async_copy(tlo, pad.at[:, pl.ds(0, 3), pl.ds(8, Z), :], sems.at[PARTS]),
        pltpu.make_async_copy(thi, pad.at[:, pl.ds(T + 3, 3), pl.ds(8, Z), :], sems.at[PARTS + 1]),
    ]
    for copy in copies + block:
        copy.start()
    for c in range(3):
        for i in range(3):
            for z, face, low, high in (
                (5 + i, zlo, corners[0], corners[2]),
                (8 + Z + i, zhi, corners[1], corners[3]),
            ):
                put_columns(pad, (c,), 0, z, low[c, i])
                put_columns(pad, (c,), 3, z, face[c, i])
                put_columns(pad, (c,), T + 3, z, high[c, i])
    for copy in copies:
        copy.wait()
    return block


PAIRS = ((0, 0), (1, 1), (2, 2), (0, 1), (0, 2), (1, 2))


def germano_pass(g, fetch, first, count, raws, filters, refs, unit=1, before=None):
    raw, last, pair, acc = refs
    _, inverse, up, down = g.lanes()
    rows = (inverse, up, down, g.kt * inverse)
    index = lax.broadcasted_iota(jnp.int32, (8, g.R), 0)

    def products(t, slot):
        for z, place in raws:
            u, s = strain_rows(fetch, t, z, g, rows)
            size = size_of(s)
            here = pl.ds(place, 8)
            for n, (a, b) in enumerate(PAIRS):
                raw[slot, n, here, :] = u[a] * u[b]
                raw[slot, 6 + n, here, :] = s[n]
                raw[slot, 12 + n, here, :] = size * s[n]

    def smooth(n, load, m):
        centre = load(1)
        h = (load(0) + load(2)) + (centre + centre)
        here = pl.ds(8 * m, 8)
        two = last[n, here, :] + h
        result = pair[n, here, :] + two
        last[n, here, :] = h
        pair[n, here, :] = two
        return result

    def contract(i, t, slot):
        for m, (z, place, keep) in enumerate(filters):
            mean = [smooth(c, lambda d, c=c: fetch(c, t, z - 1 + d), m) for c in range(3)]
            field = lambda n: smooth(
                3 + n, lambda d: raw[slot, n, place + d : place + d + 8, :], m
            )
            scaled = [f * 0.0625 for f in mean]
            leonard = [field(n) - scaled[a] * mean[b] for n, (a, b) in enumerate(PAIRS)]
            calm = [field(6 + n) for n in range(6)]
            size = size_of(calm) * (filter_ratio / 16.0)
            model = [size * calm[n] - field(12 + n) for n in range(6)]
            numer = leonard[0] * model[0]
            for n in range(1, 6):
                numer = numer + leonard[n] * model[n]
            diag = model[0] * model[0] + model[1] * model[1] + model[2] * model[2]
            side = model[3] * model[3] + model[4] * model[4] + model[5] * model[5]
            live = index < jnp.where((i >= 2) & (i < count + 2), keep, 0)
            acc[0] += jnp.where(live, numer, 0.0)
            acc[1] += jnp.where(live, diag + 0.5 * side, 0.0)

    def step(i, carry):
        if before is not None:
            before(i)
        for slot in range(unit):
            products(first - 1 + i * unit + slot, slot)
        for slot in range(unit):
            contract(i * unit + slot, first - 1 + i * unit + slot, slot)
        return carry

    lax.fori_loop(0, (count + 1 + unit) // unit, step, 0)


def row_copies(source, target, first, sems):
    part = source.shape[1] // PARTS
    return [
        pltpu.make_async_copy(
            source.at[:, pl.ds(p * part, part), :, :],
            target.at[:, pl.ds(first + p * part, part), pl.ds(0 if first == 0 else 8, source.shape[2]), :],
            sems.at[p],
        )
        for p in range(PARTS)
    ]


def inner_kernel(g, source, out, v, raw, last, pair, sems):
    copies = row_copies(source, v, 0, sems)
    for copy in copies:
        copy.start()
    out[...] = jnp.zeros_like(out)
    starts = list(range(3, g.Z - 9, 8)) + [g.Z - 9]
    part = g.T // PARTS
    copies[0].wait()

    def before(i):
        for p in range(1, PARTS):
            pl.when(i == p * part - 2)(copies[p].wait)

    germano_pass(
        g,
        lambda c, t, z: v[c, t, z : z + 8, :],
        2,
        g.T - 4,
        [(z, z - 3) for z in starts],
        [(4 + 8 * m, 8 * m, 8) for m in range(g.Z // 8 - 1)],
        (raw, last, pair, out),
        before=before,
    )


def edge_kernel(g, v, *refs):
    edges, (inner, width, out) = refs[:8], refs[8:11]
    ends, strip, raw, last, pair, acc, sems = refs[11:]
    low, high = ends.at[0], ends.at[1]
    T, Z = g.T, g.Z
    tlo, thi, zlo, zhi, *corners = edges
    wide = pl.ds(8, Z)
    pieces = (
        (v.at[:, :, pl.ds(0, 8), :], strip.at[:, pl.ds(0, T), pl.ds(8, 8), :]),
        (v.at[:, :, pl.ds(Z - 8, 8), :], strip.at[:, pl.ds(0, T), pl.ds(16, 8), :]),
        (tlo, low.at[:, pl.ds(0, 3), wide, :]),
        (v.at[:, pl.ds(0, 4), :, :], low.at[:, pl.ds(3, 4), wide, :]),
        (v.at[:, pl.ds(T - 4, 4), :, :], high.at[:, pl.ds(1, 4), wide, :]),
        (thi, high.at[:, pl.ds(5, 3), wide, :]),
    )
    copies = [pltpu.make_async_copy(a, b, sems.at[n]) for n, (a, b) in enumerate(pieces)]
    for copy in copies:
        copy.start()
    for c in range(3):
        for i in range(3):
            for n, face in enumerate((zlo, zhi)):
                put_columns(strip, (c,), 0, (5, 24)[n] + i, face[c, i])
                z = (5, 8 + Z)[n] + i
                put_columns(ends, (0, c), 0, z, corners[n][c, i])
                put_columns(ends, (0, c), 3, z, face[c, i, :4])
                put_columns(ends, (1, c), 1, z, face[c, i, T - 4 :])
                put_columns(ends, (1, c), 5, z, corners[2 + n][c, i])
    acc[...] = inner[...]
    for copy in copies:
        copy.wait()
    work = (raw, last, pair, acc)

    def near(c, t, z):
        place = z + 8 if z < Z // 2 else z - Z + 24
        return strip[c, t, place : place + 8, :]

    germano_pass(
        g,
        near,
        2,
        T - 4,
        [(-1, 0), (Z - 5, 16)],
        [(0, 0, 4), (Z - 4, 16, 4)],
        work,
        unit=SLOTS,
    )
    raws = [(8 * k - 1, 8 * k) for k in range(Z // 8 + 1)]
    filters = [(8 * m, 8 * m, 8) for m in range(Z // 8)]

    def end(which, carry):
        fetch = lambda c, t, z: ends[which, c, t + 3, z + 8 : z + 16, :]
        germano_pass(g, fetch, 0, 2, raws, filters, work)
        return carry

    lax.fori_loop(0, 2, end, 0)
    w = width[...] * (2.0 / 16.0)
    numer = jnp.sum(acc[0], axis=0, keepdims=True) * (w[:1] * (1.0 / 16.0))
    denom = jnp.sum(acc[1], axis=0, keepdims=True) * (w[:1] * w[:1])
    index = lax.broadcasted_iota(jnp.int32, (8, g.R), 0)
    out[...] = jnp.where(index == 0, numer, jnp.where(index == 1, denom, 0.0))


def source_kernel(g, v, *refs):
    edges, (width, sums, ratio), rest = refs[:8], refs[8:11], refs[11:]
    outs = rest[: g.chunks * g.ng]
    pad, tau, eddy, vt, vz, src, flip, sems, osems = rest[g.chunks * g.ng :]
    T, Z, R = g.T, g.Z, g.R
    block = fill_pad(g, v, edges, pad, sems)
    block[0].wait()
    radius, inverse, up, down = g.lanes()
    rows = (inverse, up, down, g.kt * inverse)
    kt = rows[3]
    total = jnp.sum(sums[...], axis=0)
    coefficient = total[0:1] / (total[1:2] + epsilon_den)
    strength = jnp.broadcast_to(coefficient, (8, R)) * width[...]

    fetch = lambda c, t, z: pad[c, t + 3, z + 8 : z + 16, :]

    def stress_row(t, slot):
        for zc in range(eddy.shape[1] // 8):
            _, s = strain_rows(fetch, t - 2, 8 * zc - 2, g, rows)
            e = strength * size_of(s)
            here = pl.ds(8 * zc, 8)
            eddy[t, here, :] = e * (1.0 / nu_molecular)
            side = time_step * (nu_molecular + e)
            main = side + side
            for n in range(3):
                tau[n, t, here, :] = main * s[n]
                tau[3 + n, t, here, :] = side * s[3 + n]

    def arrived(i, unit):
        for p in range(1, PARTS):
            pl.when(i == -(-(p * (T // PARTS) + 2 - unit) // unit))(block[p].wait)

    loop(T + 4, UNROLL, stress_row, arrived)

    def slab(n, t, z):
        return tau[n, t, z : z + 8, :]

    def radial(f):
        return shift_up(f) * up - shift_down(f) * down

    def turn_row(a, slot):
        t = a + 1
        for zc in range(Z // 8):
            z = 2 + 8 * zc
            rt = slab(3, t, z)
            force = (
                radial(rt)
                + (slab(1, t + 1, z) - slab(1, t - 1, z)) * kt
                + (slab(5, t, z + 1) - slab(5, t, z - 1)) * g.kz
                + rt * (inverse + inverse)
            )
            vt[a, pl.ds(8 * zc, 8), :] = pad[1, a + 2, 8 + 8 * zc : 16 + 8 * zc, :] + force

    loop(T + 2, UNROLL, turn_row)
    r_up = shift_up(radius) * inverse * up
    r_down = shift_down(radius) * inverse * down

    def axial_row(a, slot):
        t = a + 2
        for zc in range(vz.shape[1] // 8):
            z = 1 + 8 * zc
            rz = slab(4, t, z)
            force = (
                radial(rz)
                + (slab(5, t + 1, z) - slab(5, t - 1, z)) * kt
                + (slab(2, t, z + 1) - slab(2, t, z - 1)) * g.kz
                + rz * inverse
            )
            vz[a, pl.ds(8 * zc, 8), :] = pad[2, a + 3, 7 + 8 * zc : 15 + 8 * zc, :] + force

    loop(T, UNROLL, axial_row)

    def radial_row(a, slot):
        t = a + 2
        for zc in range(Z // 8):
            z = 2 + 8 * zc
            rr = slab(0, t, z)
            force = (
                radial(rr)
                + (slab(3, t + 1, z) - slab(3, t - 1, z)) * kt
                + (slab(4, t, z + 1) - slab(4, t, z - 1)) * g.kz
                + (rr - slab(1, t, z)) * inverse
            )
            src[a, pl.ds(8 * zc, 8), :] = pad[0, a + 3, 8 + 8 * zc : 16 + 8 * zc, :] + force
            ratio[a, pl.ds(8 * zc, 8), :] = eddy[t, z : z + 8, :]

    loop(T, UNROLL, radial_row)

    def source_row(a, slot):
        for zc in range(Z // 8):
            here = pl.ds(8 * zc, 8)
            vr = src[a, here, :]
            src[a, here, :] = (
                shift_up(vr) * r_up
                - shift_down(vr) * r_down
                + (vt[a + 2, here, :] - vt[a, here, :]) * kt
                + (vz[a, 8 * zc + 2 : 8 * zc + 10, :] - vz[a, 8 * zc : 8 * zc + 8, :]) * g.kz
            )

    loop(T, UNROLL, source_row)
    flat = src.reshape(T * src.shape[1], R)
    turned = flip.reshape(R * flip.shape[1], 2 * T)

    def flip_step(p, slot):
        even = flat[pl.ds(2 * p, T, stride=src.shape[1]), :]
        odd = flat[pl.ds(2 * p + 1, T, stride=src.shape[1]), :]
        turned[pl.ds(p, R, stride=flip.shape[1]), :] = jnp.concatenate([even, odd], axis=0).T

    loop(Z // 2, UNROLL, flip_step)
    me = lax.axis_index("gz")
    copies = []
    for c in range(g.chunks):
        for s in range(g.ng):
            first = g.ng * g.first[c] + lax.rem(me + s, g.ng) * g.rb[c]
            n = c * g.ng + s
            copies.append(
                pltpu.make_async_copy(
                    flip.at[pl.ds(first, g.rb[c]), pl.ds(0, Z // 2), :], outs[n], osems.at[n]
                )
            )
    for copy in copies:
        copy.start()
    for copy in copies:
        copy.wait()


def split(x):
    parts = []
    for _ in range(2):
        parts.append(x.astype(jnp.bfloat16))
        x = x - parts[-1].astype(jnp.float32)
    return parts + [x.astype(jnp.bfloat16)]


def split_table(x):
    parts = []
    for _ in range(2):
        high = lax.reduce_precision(x, 8, 7)
        parts.append(high.astype(jnp.bfloat16))
        x = x - high
    return parts + [x.astype(jnp.bfloat16)]


def dot6(a, b):
    dot = functools.partial(jnp.dot, preferred_element_type=jnp.float32)
    small = dot(a[1], b[1]) + dot(a[2], b[0]) + dot(a[0], b[2])
    return dot(a[0], b[0]) + (dot(a[1], b[0]) + dot(a[0], b[1]) + small)


def axial_kernel(g, rb, *refs):
    blocks, tables = refs[: g.ng], refs[g.ng : g.ng + 3]
    outs = refs[g.ng + 3 : g.ng + 3 + g.nt]
    left = refs[g.ng + 3 + g.nt :]
    T, zp, kb = g.T, g.Z // 2, g.kb
    mine, other = lax.axis_index("gz"), lax.axis_index("theta")
    for s in range(g.ng):
        source = lax.rem(mine + g.ng - s, g.ng)
        for d in range(g.nt):
            target = lax.rem(other + d, g.nt)
            here = (pl.ds(d * kb, kb), pl.ds(4 * zp * s, 4 * zp))
            for n in range(3):
                left[n][here] = tables[n][source, target]
    per = 2 if rb % 2 == 0 else 1
    first = lax.broadcasted_iota(jnp.int32, (zp, 2 * T), 1) < T

    def column(r):
        parts = []
        for s in range(g.ng):
            x = blocks[s][r]
            y = jnp.concatenate([x[:, T:], x[:, :T]], axis=1)
            for f in (x, y):
                parts.append(jnp.where(first, f, 0.0))
                parts.append(jnp.where(first, 0.0, f))
        return jnp.concatenate(parts, axis=0)

    def step(i, carry):
        right = jnp.concatenate([column(per * i + q) for q in range(per)], axis=1)
        result = dot6([w[...] for w in left], split(right))
        for q in range(per):
            for d in range(g.nt):
                outs[d][per * i + q] = result[d * kb : (d + 1) * kb, q * 2 * T : (q + 1) * 2 * T]
        return carry

    lax.fori_loop(0, rb // per, step, 0)


def turn_kernel(g, rb, *refs):
    blocks, tables = refs[: g.nt], refs[g.nt : g.nt + 3]
    outs = refs[g.nt + 3 : g.nt + 3 + g.ng]
    mine, other = lax.axis_index("theta"), lax.axis_index("gz")
    rows = rb * g.kb
    left = split(jnp.concatenate([b[...].reshape(rows, 2 * g.T) for b in blocks], axis=1))
    for d in range(g.ng):
        target = lax.rem(other + d, g.ng)
        source = [lax.rem(mine + g.nt - s, g.nt) for s in range(g.nt)]
        right = [jnp.concatenate([w[target, s] for s in source], axis=0) for w in tables]
        result = dot6(left, right)
        for c in range(2):
            part = result[:, c * g.mb : (c + 1) * g.mb]
            outs[d][c] = part.reshape(rb, g.kb, g.mb)


def solve_kernel(g, *refs):
    count = g.chunks * g.ng
    blocks, coefs, out = refs[:count], refs[count], refs[count + 1]
    data, factor, flip, sems, osems = refs[count + 2 :]
    R, kb, mb = g.R, g.kb, g.mb
    mine, other = lax.axis_index("gz"), lax.axis_index("theta")
    copies = []
    for c in range(g.chunks):
        for s in range(g.ng):
            first = g.ng * g.first[c] + lax.rem(mine + g.ng - s, g.ng) * g.rb[c]
            n = c * g.ng + s
            copies.append(
                pltpu.make_async_copy(
                    blocks[n], data.at[:, pl.ds(first, g.rb[c]), pl.ds(0, kb), :], sems.at[n]
                )
            )
    for copy in copies:
        copy.start()
    m = mine * mb + lax.broadcasted_iota(jnp.int32, (kb, mb), 1)
    k = other * kb + lax.broadcasted_iota(jnp.int32, (kb, mb), 0)
    a = jnp.minimum(m, g.NTH - m).astype(jnp.float32)
    q = jnp.minimum(k, g.NZ - k).astype(jnp.float32) * (2.0 * math.pi / pipe_length)
    a2, q2 = a * a, q * q
    zero = jnp.zeros((kb, mb), jnp.float32)

    def forward(r, carry):
        cp, re, im = carry
        lower, upper, centre, inv2 = (coefs[n, r] for n in range(4))
        w = 1.0 / ((centre - q2) - a2 * inv2 - lower * cp)
        cp = upper * w
        re = (data[0, r, :kb, :] - lower * re) * w
        im = (data[1, r, :kb, :] - lower * im) * w
        factor[r] = cp
        data[0, r, :kb, :] = re
        data[1, r, :kb, :] = im
        return cp, re, im

    state = (zero, zero, zero)
    for c in range(g.chunks):
        for copy in copies[c * g.ng : (c + 1) * g.ng]:
            copy.wait()
        start = g.ng * g.first[c]
        state = lax.fori_loop(start, start + g.ng * g.rb[c], forward, state, unroll=4)

    def backward(i, carry):
        re, im = carry
        r = R - 1 - i
        cp = factor[r]
        re = data[0, r, :kb, :] - cp * re
        im = data[1, r, :kb, :] - cp * im
        data[0, r, :kb, :] = re
        data[1, r, :kb, :] = im
        return re, im

    lax.fori_loop(0, R, backward, (zero, zero), unroll=4)
    flat = data.reshape(2 * R * data.shape[2], mb)
    turned = flip.reshape(2 * mb * flip.shape[2], R)
    stores = []
    for c in range(2):

        def flip_step(i, slot, c=c):
            rows = flat[pl.ds(c * R * data.shape[2] + i, R, stride=data.shape[2]), :]
            turned[pl.ds(c * mb * flip.shape[2] + i, mb, stride=flip.shape[2]), :] = rows.T

        loop(kb, UNROLL, flip_step)
        copy = pltpu.make_async_copy(flip.at[c, :, pl.ds(0, kb), :], out.at[c], osems.at[c])
        copy.start()
        stores.append(copy)
    for copy in stores:
        copy.wait()


def exchange(blocks, axis):
    count = len(blocks)
    received = [blocks[0]]
    for s in range(1, count):
        ring = [(i, (i + s) % count) for i in range(count)]
        received.append(lax.ppermute(blocks[s], axis, ring))
    return received


def after(later, earlier):
    joined = lax.optimization_barrier((list(later), list(earlier)))
    return joined[0], joined[1]


def halo(g, v):
    T, Z = g.T, g.Z

    def move(block, dt, dz):
        ring = [
            (t * g.ng + z, (t + dt) % g.nt * g.ng + (z + dz) % g.ng)
            for t in range(g.nt)
            for z in range(g.ng)
        ]
        return lax.ppermute(block, ("theta", "gz"), ring)

    first = v[:, :, :3].transpose(0, 2, 1, 3)
    final = v[:, :, Z - 3 :].transpose(0, 2, 1, 3)
    faces = [
        move(final, 0, 1), move(first, 0, -1), move(v[:, T - 3 :], 1, 0), move(v[:, :3], -1, 0)
    ]
    corners = [
        move(final[:, :, T - 3 :], 1, 1),
        move(first[:, :, T - 3 :], 1, -1),
        move(final[:, :, :3], -1, 1),
        move(first[:, :, :3], -1, -1),
    ]
    return faces[2], faces[3], faces[0], faces[1], *corners


def axial_table(g):
    z, k = np.arange(g.NZ), np.arange(g.NZ)
    angle = 2.0 * math.pi * ((k[:, None] * z[None, :]) % g.NZ) / g.NZ
    scale = 1.0 / math.sqrt(g.NTH * g.NZ)
    cos = (np.cos(angle) * scale).reshape(g.nt, g.kb, g.ng, g.Z // 2, 2)
    sin = (-np.sin(angle) * scale).reshape(g.nt, g.kb, g.ng, g.Z // 2, 2)
    parts = [cos[..., 0], sin[..., 1], cos[..., 1], sin[..., 0]]
    table = np.stack(parts, axis=3).reshape(g.nt, g.kb, g.ng, 2 * g.Z)
    return split_table(jnp.asarray(table.transpose(2, 0, 1, 3).astype(np.float32)))


def turn_table(g):
    t, m = np.arange(g.T), np.arange(g.NTH)
    base = 2.0 * math.pi * ((t[:, None] * m[None, :]) % g.NTH) / g.NTH
    skip = 2.0 * math.pi * ((np.arange(g.nt)[:, None] * g.T * m[None, :]) % g.NTH) / g.NTH
    f32 = lambda x: jnp.asarray(x.astype(np.float32))
    fold = lambda x: x.reshape(x.shape[0], g.ng, g.mb).transpose(1, 0, 2)
    c0, s0 = f32(fold(np.cos(base)))[:, None], f32(fold(np.sin(base)))[:, None]
    c1, s1 = f32(fold(np.cos(skip)))[:, :, None], f32(fold(np.sin(skip)))[:, :, None]
    cos = c0 * c1 - s0 * s1
    sin = s0 * c1 + c0 * s1
    top = jnp.concatenate([cos, -sin], axis=-1)
    bottom = jnp.concatenate([sin, cos], axis=-1)
    return split_table(jnp.concatenate([top, bottom], axis=-2))


def solve_coefs(g):
    R = g.R
    radius = (np.arange(R) + 0.5) / R
    lower = (radius - 0.5 / R) / radius * (R * R)
    upper = (radius + 0.5 / R) / radius * (R * R)
    last = np.arange(R) == R - 1
    centre = -(lower + upper) - np.where(last, upper, 0.0)
    upper = np.where(last, 0.0, upper)
    return jnp.asarray(np.stack([lower, upper, centre, 1.0 / radius**2]).astype(np.float32))


def body(velocity):
    return program(Grid(velocity), velocity)


def program(g, velocity):
    T, Z, R, kb, mb = g.T, g.Z, g.R, g.kb, g.mb
    f32 = jnp.float32
    shape = lambda *s: jax.ShapeDtypeStruct(s, f32)
    buf = lambda *s: pltpu.VMEM(s, f32)
    dma = pltpu.SemaphoreType.DMA
    edges = halo(g, velocity)
    width = width_row(g)
    pad = buf(3, T + 6, odd_tiles(Z + 16), R)
    halo_specs = [ANY, ANY, ANY] + [VM] * 6
    work = [buf(SLOTS, 18, odd_tiles(Z + 2), R), buf(21, odd_tiles(Z), R), buf(21, odd_tiles(Z), R)]
    inner = pl.pallas_call(
        functools.partial(inner_kernel, g),
        out_shape=shape(2, 8, R),
        in_specs=[ANY],
        out_specs=VM,
        scratch_shapes=[buf(3, T, Z, R), *work, dma((PARTS,))],
        compiler_params=params(50 * 1024 * 1024),
        name="inner_sums",
    )(velocity)
    part = pl.pallas_call(
        functools.partial(edge_kernel, g),
        out_shape=shape(8, R),
        in_specs=[ANY, ANY, ANY] + [VM] * 8,
        out_specs=VM,
        scratch_shapes=[
            buf(2, 3, 8, odd_tiles(Z + 16), R),
            buf(3, T + 2, 40, R),
            *work,
            buf(2, 8, R),
            dma((6,)),
        ],
        compiler_params=params(40 * 1024 * 1024),
        name="edge_sums",
    )(velocity, *edges, inner, width)
    count = g.nt * g.ng
    sums = lax.all_to_all(
        jnp.broadcast_to(part[None], (count, 8, R)), ("theta", "gz"), 0, 0, tiled=True
    )
    outs = pl.pallas_call(
        functools.partial(source_kernel, g),
        out_shape=[shape(T, Z, R)]
        + [shape(rb, Z // 2, 2 * T) for rb in g.rb for _ in range(g.ng)],
        in_specs=halo_specs + [VM] * 2,
        out_specs=[VM] + [ANY] * (g.chunks * g.ng),
        scratch_shapes=[
            pad,
            buf(6, T + 5, odd_tiles(Z + 10), R),
            buf(T + 4, round_up(Z + 4, 8), R),
            buf(T + 2, odd_tiles(Z), R),
            buf(T, round_up(Z + 2, 8), R),
            buf(T, Z + 8, R),
            buf(R, Z // 2 + 8, 2 * T),
            dma((PARTS + 2,)),
            dma((g.chunks * g.ng,)),
        ],
        compiler_params=params(),
        name="source",
    )(velocity, *edges, width, sums)
    ratio, pieces = outs[0], outs[1:]
    axial_tables = axial_table(g)
    turn_tables = turn_table(g)
    axials, modes = [], []
    for c, rb in enumerate(g.rb):
        piece = pieces[c * g.ng : (c + 1) * g.ng]
        if c >= 1:
            piece, axials[c - 1] = after(piece, axials[c - 1])
        line = exchange(piece, "gz")
        axial = pl.pallas_call(
            functools.partial(axial_kernel, g, rb),
            out_shape=[shape(rb, kb, 2 * T)] * g.nt,
            in_specs=[VM] * (g.ng + 3),
            out_specs=[VM] * g.nt,
            scratch_shapes=[pltpu.VMEM((g.NZ, 2 * g.NZ), jnp.bfloat16)] * 3,
            compiler_params=params(24 * 1024 * 1024),
            name="axial_modes",
        )(*line, *axial_tables)
        axials.append(axial)
    for c, rb in enumerate(g.rb):
        cycle = exchange(axials[c], "theta")
        turned = pl.pallas_call(
            functools.partial(turn_kernel, g, rb),
            out_shape=[shape(2, rb, kb, mb)] * g.ng,
            in_specs=[VM] * (g.nt + 3),
            out_specs=[VM] * g.ng,
            compiler_params=params(40 * 1024 * 1024),
            name="turn_modes",
        )(*cycle, *turn_tables)
        modes += exchange(turned, "gz")
    pressure = pl.pallas_call(
        functools.partial(solve_kernel, g),
        out_shape=shape(2, mb, kb, R),
        in_specs=[ANY] * len(modes) + [pl.BlockSpec(memory_space=pltpu.SMEM)],
        out_specs=ANY,
        scratch_shapes=[
            buf(2, R, kb + 8, mb),
            buf(R, kb, mb),
            buf(2, mb, kb + 8, R),
            dma((len(modes),)),
            dma((2,)),
        ],
        compiler_params=params(40 * 1024 * 1024),
        name="solve_modes",
    )(*modes, solve_coefs(g))
    return (ratio, pressure)


def solution(mesh):
    return jax.shard_map(
        body,
        mesh=mesh,
        in_specs=(P(None, "theta", "gz", None),),
        out_specs=(P("theta", "gz", None), P(None, "gz", "theta", None)),
        check_vma=False,
    )
```
